256 devices in a mesh: strike: 32 (over y_lo, z, core), depth: 8 (over x, y_hi).
Axes of the slice: x: 4, y: 4 (y_hi: 2, y_lo: 2; y = y_hi * 2 + y_lo), z: 8, core: 2. Of those that a mesh axis runs over, the one named last changes fastest.
Arguments:
- velocity: float32 [3, 64, 32, 4096], P(None, 'depth', None, 'strike'), may hold values from -6 to 6
- stress: float32 [6, 64, 32, 4096], P(None, 'depth', None, 'strike'), may hold values from -6 to 6
- buoyancy: float32 [64, 32, 4096], P('depth', None, 'strike'), may hold values from 0.5 to 1
- lame_lambda: float32 [64, 32, 4096], P('depth', None, 'strike'), may hold values from 0.3 to 0.8
- shear_modulus: float32 [64, 32, 4096], P('depth', None, 'strike'), may hold values from 0.3 to 0.8
- past_rates: float32 [64, 64, 4096], P(None, 'depth', 'strike'), may hold values from -6 to 6
- memory_coefs: float32 [64], replicated, may hold values from 0.02 to 0.2
- prestress: float32 [64, 4096], P('depth', 'strike'), may hold values from -6 to 6
- fault_mask: int32 [64, 4096], P('depth', 'strike'), may hold values 0 or 1
Outputs:
- velocity_out: float32 [3, 64, 32, 4096], P(None, 'depth', None, 'strike')
- stress_out: float32 [6, 64, 32, 4096], P(None, 'depth', None, 'strike')
The draws below stay inside these ranges and needn't reach their ends.
All inputs are finite; a program needn't handle non-finite values. No bound on the sum of `fault_mask` on one device may be relied on, other than what follows from the above.
Results may differ from the reference program's by a relative error of at most 0.0001.
Values sent between devices are 32-bit elements; how exact they have to be, the bound alone decides.
No kernel may reach another device: no remote copies, remote signals or barrier semaphores. Data moves between devices by JAX's collectives and lax.ppermute only.
A program may use at most 64 MiB of HBM per device.

```python
import math
import jax
import jax.numpy as jnp
from jax import lax

CX = 128
NY = 32
HIST = 64
STEPS = 8
NX = 4096
NZ = 64


def with_ends(entries, rng, smallest, top_value):
    shape = entries.shape
    place = [jax.random.randint(jax.random.fold_in(rng, axis), (), 0, shape[axis]) for axis in range(len(shape))]
    entries = entries.at[tuple(place)].set(smallest)
    longest = shape.index(max(shape))
    place[longest] = (place[longest] + 1) % shape[longest]
    return entries.at[tuple(place)].set(top_value)


def block_scale(rng, shape, split, smallest, largest):
    loudness = 1.0
    for dim, parts in split:
        steps = jax.random.uniform(jax.random.fold_in(jax.random.fold_in(rng, 6), dim), (parts,), jnp.float32, smallest / len(split), largest / len(split))
        loudness = loudness * jnp.repeat(jnp.exp(steps), shape[dim] // parts).reshape((-1,) + (1,) * (len(shape) - 1 - dim))
    return loudness


def noise(rng, shape, deviation, reach, shards=(), dtype=jnp.bfloat16):
    loudness = block_scale(rng, shape, shards, -0.22, 0.18) if shards else 1.0
    result = jax.random.normal(rng, shape, jnp.float32) * deviation * loudness
    return jnp.minimum(jnp.maximum(result, -reach), reach).astype(dtype)


def setup_inputs(seed: int = 0) -> dict:
    key_of = jax.random.split(jax.random.key(seed), 10)
    return {
        "velocity": noise(key_of[0], (3, NZ, NY, NX), 1.0, 6.0, ((1, 8), (3, 32)), jnp.float32),
        "stress": noise(key_of[1], (6, NZ, NY, NX), 1.0, 6.0, ((1, 8), (3, 32)), jnp.float32),
        "buoyancy": jnp.clip(jnp.exp(math.log(1.0) - 0.6931472 * jax.random.uniform(key_of[2], (NZ, NY, NX), jnp.float32) ** block_scale(key_of[2], (NZ, NY, NX), ((0, 8), (2, 32)), -0.2, 0.2)), 0.5, 1.0),
        "lame_lambda": jnp.clip(jnp.exp(math.log(0.8) - 0.98082923 * jax.random.uniform(key_of[3], (NZ, NY, NX), jnp.float32) ** block_scale(key_of[3], (NZ, NY, NX), ((0, 8), (2, 32)), -0.2, 0.2)), 0.3, 0.8),
        "shear_modulus": jnp.clip(jnp.exp(math.log(0.8) - 0.98082923 * jax.random.uniform(key_of[4], (NZ, NY, NX), jnp.float32) ** block_scale(key_of[4], (NZ, NY, NX), ((0, 8), (2, 32)), -0.2, 0.2)), 0.3, 0.8),
        "past_rates": noise(key_of[5], (HIST, NZ, NX), 1.0, 6.0, ((1, 8), (2, 32)), jnp.float32),
        "memory_coefs": jnp.clip(jnp.exp(jax.random.uniform(key_of[6], (HIST,), jnp.float32, math.log(0.02), math.log(0.2))), 0.02, 0.2),
        "prestress": noise(key_of[7], (NZ, NX), 1.0, 6.0, ((0, 8), (1, 32)), jnp.float32),
        "fault_mask": with_ends((jax.random.randint(key_of[8], (NZ, NX), 0, 4) < 3).astype(jnp.int32), jax.random.fold_in(key_of[8], 1), 0, 1),
    }


DT = 0.3
FRIC = 0.5


def ahead_x(f):
    return jnp.roll(f, -1, 2)


def behind_x(f):
    return jnp.roll(f, 1, 2)


def ahead_y(f):
    return jnp.concatenate([f[:, 1:], jnp.zeros_like(f[:, :1])], axis=1)


def behind_y(f):
    return jnp.concatenate([jnp.zeros_like(f[:, :1]), f[:, :-1]], axis=1)


def ahead_z(f):
    return jnp.concatenate([f[1:], jnp.zeros_like(f[:1])], axis=0)


def behind_z(f):
    return jnp.concatenate([jnp.zeros_like(f[:1]), f[:-1]], axis=0)


def reference(velocity, stress, buoyancy, lame_lambda, shear_modulus, past_rates, memory_coefs, prestress, fault_mask):
    vx, vy, vz = velocity[0], velocity[1], velocity[2]
    sxx, sxy, sxz, syz, szz, syy = stress[0], stress[1], stress[2], stress[3], stress[4], stress[5]
    center = vx.shape[1] // 2
    stiff = lame_lambda + 2.0 * shear_modulus
    history = past_rates
    for step in range(STEPS):
        vx = vx + DT * buoyancy * ((ahead_x(sxx) - sxx) + (sxy - behind_y(sxy)) + (sxz - behind_z(sxz)))
        vy = vy + DT * buoyancy * ((sxy - behind_x(sxy)) + (ahead_y(syy) - syy) + (syz - behind_z(syz)))
        vz = vz + DT * buoyancy * ((sxz - behind_x(sxz)) + (syz - behind_y(syz)) + (ahead_z(szz) - szz))
        rate = vx[:, center + 1, :] - vx[:, center, :]
        memory = jnp.tensordot(memory_coefs, history, axes=1, precision=lax.Precision.HIGHEST)
        strain_x = vx - behind_x(vx)
        strain_y = vy - behind_y(vy)
        strain_z = vz - behind_z(vz)
        sxx = sxx + DT * (stiff * strain_x + lame_lambda * (strain_y + strain_z))
        syy = syy + DT * (stiff * strain_y + lame_lambda * (strain_x + strain_z))
        szz = szz + DT * (stiff * strain_z + lame_lambda * (strain_x + strain_y))
        sxy = sxy + DT * shear_modulus * ((ahead_y(vx) - vx) + (ahead_x(vy) - vy))
        sxz = sxz + DT * shear_modulus * ((ahead_z(vx) - vx) + (ahead_x(vz) - vz))
        syz = syz + DT * shear_modulus * ((ahead_z(vy) - vy) + (ahead_y(vz) - vz))
        fault = jnp.where(fault_mask == 1, prestress + FRIC * rate - memory, sxy[:, center, :])
        sxy = sxy.at[:, center, :].set(fault)
        if step + 1 < STEPS:
            history = jnp.roll(jnp.concatenate([rate[None], history[:-1]], axis=0), CX, axis=2)
    return jnp.stack([vx, vy, vz]), jnp.stack([sxx, sxy, sxz, syz, szz, syy])
```

```python
import functools

import jax
import jax.numpy as jnp
from jax import lax
from jax.experimental import pallas as pl
from jax.experimental.pallas import tpu as pltpu
from jax.sharding import PartitionSpec as P

HIST = 64
STEPS = 8
DT = 0.3
FRIC = 0.5

NY = 32
Y0 = NY // 2
LANES = 128
EXT = 2 * LANES
W = STEPS
ROWS = 16
VMEM = pl.BlockSpec(memory_space=pltpu.VMEM)
SMEM = pl.BlockSpec(memory_space=pltpu.SMEM)

VX, VY, VZ, SXX, SXZ, SYZ, SZZ, SYY, SXY, B, LAM, MU = range(12)

UP = ((VX, 2), (VX, 3), (VY, 2), (VY, 3), (VZ, 2), (SXX, 2), (SXZ, 2), (SYZ, 2), (SZZ, 2), (SYY, 2), (SXY, 2))
DOWN = ((VX, 9), (VY, 9), (VZ, 8), (VZ, 9), (SXZ, 9), (SYZ, 9), (SZZ, 9))
UP_TO = tuple((f, z + 8) for f, z in UP)
DOWN_TO = tuple((f, z - 8) for f, z in DOWN)
UP_FIRST = UP + ((B, 2), (LAM, 2), (MU, 2))
DOWN_FIRST = DOWN + ((B, 9), (LAM, 9), (MU, 9))


def tiles(planes):
    return len(planes) + -(-len(planes) // 8)


def call(body, outs, ins, aliases=None, smem=()):
    return pl.pallas_call(
        body,
        out_shape=[jax.ShapeDtypeStruct(s, jnp.float32) for s in outs],
        in_specs=[SMEM if i in smem else VMEM for i in range(len(ins))],
        out_specs=[VMEM] * len(outs),
        input_output_aliases=aliases or {},
        compiler_params=pltpu.CompilerParams(vmem_limit_bytes=32 * 1024 * 1024),
        cost_estimate=pl.CostEstimate(flops=4_000_000, bytes_accessed=4_000_000, transcendentals=0),
    )(*ins)


def lane_of(rows):
    return lax.broadcasted_iota(jnp.int32, (rows, LANES), 1)


def rolled(tile, by):
    by %= LANES
    return tile if by == 0 else pltpu.roll(tile, by, 1)


def ahead_x(f):
    return pltpu.roll(f, f.shape[1] - 1, 1)


def behind_x(f):
    return pltpu.roll(f, 1, 1)


def ahead_y(f):
    row = lax.broadcasted_iota(jnp.int32, f.shape, 0)
    return jnp.where(row == NY - 1, 0.0, pltpu.roll(f, NY - 1, 0))


def behind_y(f):
    row = lax.broadcasted_iota(jnp.int32, f.shape, 0)
    return jnp.where(row == 0, 0.0, pltpu.roll(f, 1, 0))


def plane_of(refs, f, z):
    v, s, q, m = refs
    if f < SXX:
        return v.at[f, z]
    if f < SXY:
        return s.at[f - SXX, z]
    if f == SXY:
        return q.at[z]
    return m.at[f - B, z - 2]


def velocity_change(stress, z, b, want):
    sxy, sxz, syz, szz = stress(SXY, z), stress(SXZ, z), stress(SYZ, z), stress(SZZ, z)
    out = {}
    if VX in want:
        sxx = stress(SXX, z)
        out[VX] = b * ((ahead_x(sxx) - sxx) + (sxy - behind_y(sxy)) + (sxz - stress(SXZ, z - 1)))
    if VY in want:
        syy = stress(SYY, z)
        out[VY] = b * ((sxy - behind_x(sxy)) + (ahead_y(syy) - syy) + (syz - stress(SYZ, z - 1)))
    if VZ in want:
        out[VZ] = b * ((sxz - behind_x(sxz)) + (syz - behind_y(syz)) + (stress(SZZ, z + 1) - szz))
    return out


def stress_change(v, z, lam, mu, want):
    vx, vy, vz = v[VX, z], v[VY, z], v[VZ, z]
    ex = vx - behind_x(vx)
    ey = vy - behind_y(vy)
    ez = vz - v[VZ, z - 1]
    spread = lam * (ex + ey + ez)
    twice = mu + mu
    out = {}
    if SXX in want:
        out[SXX] = spread + twice * ex
        out[SYY] = spread + twice * ey
        out[SXY] = mu * ((ahead_y(vx) - vx) + (ahead_x(vy) - vy))
    out[SZZ] = spread + twice * ez
    out[SXZ] = mu * ((v[VX, z + 1] - vx) + (ahead_x(vz) - vz))
    out[SYZ] = mu * ((v[VY, z + 1] - vy) + (ahead_y(vz) - vz))
    return out


ALL_V = (VX, VY, VZ)
ALL_S = (SXX, SXZ, SYZ, SZZ, SYY, SXY)


def rate_at(v, z):
    return v[VX, z, Y0 + 1 : Y0 + 2, :] - v[VX, z, Y0 : Y0 + 1, :]


def slide(q, fp, z, traction):
    slides = fp[1, pl.ds(z, 1), :] > 0.5
    q[z, Y0 : Y0 + 1, :] = jnp.where(slides, traction, q[z, Y0 : Y0 + 1, :])


def pack(refs, planes, out):
    lane = lane_of(NY)
    for first in range(0, len(planes), 8):
        edges = jnp.zeros((NY, LANES), jnp.float32)
        for i, (f, z) in enumerate(planes[first : first + 8]):
            ref = plane_of(refs, f, z)
            out[first + i] = ref[:, :LANES]
            moved = rolled(ref[:, LANES:], W + 2 * W * i)
            edges = jnp.where((lane >= 2 * W * i) & (lane < 2 * W * (i + 1)), moved, edges)
        out[len(planes) + first // 8] = edges


def unpacked(got, planes, i, rows=slice(None)):
    edges = got[len(planes) + i // 8, rows, :]
    return jnp.concatenate([got[i, rows, :], rolled(edges, -(W + 2 * W * (i % 8)))], axis=1)


def edges_kernel(coefs, past, vel, str_, b, lam, mu, pre, mask, to_next, to_prev, owed):
    lane8 = lane_of(8)
    sums = [None] * STEPS
    for j in range(STEPS):
        parts = [None] * 4
        for k in range(HIST - j):
            term = coefs[j + k] * past[k]
            parts[k % 4] = term if parts[k % 4] is None else parts[k % 4] + term
        sums[j] = (parts[0] + parts[1]) + (parts[2] + parts[3])
        owed[j] = sums[j]
    nxt = jnp.zeros((8, LANES), jnp.float32)
    prv = jnp.zeros((8, LANES), jnp.float32)
    for i, plane in enumerate(sums + [pre[...], mask[...]]):
        here = (lane8 >= W * i) & (lane8 < W * (i + 1))
        nxt = jnp.where(here, rolled(plane, W * i - (LANES - W)), nxt)
        prv = jnp.where(here, rolled(plane, W * i), prv)
    to_next[6] = jnp.zeros((NY, LANES), jnp.float32)
    to_prev[6] = jnp.zeros((NY, LANES), jnp.float32)
    to_next[6, 0:8, :] = nxt
    to_prev[6, 0:8, :] = prv
    lane = lane_of(NY)
    fields = [(vel, f) for f in range(3)] + [(str_, f) for f in range(6)] + [(b, None), (lam, None), (mu, None)]
    for t in range(6):
        nxt = jnp.zeros((NY, LANES), jnp.float32)
        prv = jnp.zeros((NY, LANES), jnp.float32)
        for i in range(16):
            ref, f = fields[2 * t + i // 8]
            plane = ref[i % 8] if f is None else ref[f, i % 8]
            here = (lane >= W * i) & (lane < W * (i + 1))
            nxt = jnp.where(here, rolled(plane, W * i - (LANES - W)), nxt)
            prv = jnp.where(here, rolled(plane, W * i), prv)
        to_next[t] = nxt
        to_prev[t] = prv


def move_first(refs, z, q_now=None):
    v, s, q, m = refs

    def stress(f, at):
        return (q if q_now is None else q_now)[at] if f == SXY else s[f - SXX, at]

    return velocity_change(stress, z, m[0, z - 2], ALL_V)


def start_kernel(vel, str_, b, lam, mu, pre, mask, owed, from_prev, from_next, v, s, q, m, fp, lists, up, down):
    lane = lane_of(NY)
    lane8 = lane_of(8)
    empty = jnp.zeros((NY, EXT), jnp.float32)
    s[SXZ - SXX, 1] = empty
    s[SYZ - SXX, 1] = empty
    s[SZZ - SXX, 10] = empty
    refs = (v, s, q, m)
    fields = [(vel, f, f) for f in range(3)] + [(str_, i, f) for i, f in enumerate((SXX, SXY, SXZ, SYZ, SZZ, SYY))]
    fields += [(b, None, B), (lam, None, LAM), (mu, None, MU)]
    for k, (ref, i, f) in enumerate(fields):
        for z in range(8):
            at = (k % 2) * 8 + z
            plane = ref[z] if i is None else ref[i, z]
            edge = jnp.where(
                lane < LANES // 2,
                rolled(from_next[k // 2], -W * at),
                rolled(from_prev[k // 2], LANES - W - W * at),
            )
            if f >= B:
                plane, edge = DT * plane, DT * edge
            to = plane_of(refs, f, z + 2)
            to[:, :LANES] = plane
            to[:, LANES:] = edge
    fp[...] = jnp.zeros_like(fp)
    lists[...] = jnp.zeros_like(lists)
    for i in range(STEPS + 2):
        plane = owed[i] if i < STEPS else (pre, mask)[i - STEPS][...]
        edge = jnp.where(
            lane8 < LANES // 2,
            rolled(from_next[6, 0:8, :], -W * i),
            rolled(from_prev[6, 0:8, :], LANES - W - W * i),
        )
        to, j = (lists, i) if i < STEPS else (fp, i - STEPS)
        to[j, 2:10, :LANES] = plane
        to[j, 2:10, LANES:] = edge

    def step(z, carry):
        for f, change in move_first(refs, z).items():
            v[f, z] += change
        return carry

    lax.fori_loop(2, 10, step, 0)
    pack(refs, UP_FIRST, up)
    pack(refs, DOWN_FIRST, down)
    last = tiles(UP_FIRST)
    up[last] = jnp.zeros((NY, LANES), jnp.float32)
    for i in range(STEPS + 2):
        to, j = (lists, i) if i < STEPS else (fp, i - STEPS)
        up[last, i : i + 1, :] = to[j, 2:3, :LANES]
        up[last, 16 + i : 17 + i, :] = to[j, 2:3, LANES:]


def meet_kernel(first, coefs, got_up, got_down, v, s, m, edge_m, fp, lists, sent, *more):
    up, down = (UP_FIRST, DOWN_FIRST) if first else (UP, DOWN)
    if first:
        edge_out, fp_out, lists_out = more
        for k in range(3):
            edge_out[k, 0] = unpacked(got_down, down, down.index((B + k, 9)))
            edge_out[k, 1] = unpacked(got_up, up, up.index((B + k, 2)))
        fp_out[...] = fp[...]
        lists_out[...] = lists[...]
        last = tiles(up)
        for i in range(STEPS + 2):
            to, j = (lists_out, i) if i < STEPS else (fp_out, i - STEPS)
            to[j, 10:11, :LANES] = got_up[last, i : i + 1, :]
            to[j, 10:11, LANES:] = got_up[last, 16 + i : 17 + i, :]
        edge_m, lists = edge_out, lists_out
    rows = slice(Y0, Y0 + 8)
    for z in range(2, 11):
        if z < 10:
            vx = v[VX, z, rows, :]
        else:
            vx = unpacked(got_up, up, up.index((VX, 2)), rows) - edge_m[0, 1, rows, :] * s[SXZ - SXX, 9, rows, :]
        if z == 2:
            vx = vx - m[0, 0, rows, :] * unpacked(got_down, down, down.index((SXZ, 9)), rows)
        rate = vx[1:2, :] - vx[0:1, :]
        for j in range(lists.shape[0] - 1):
            sent[j, z : z + 1, :] = lists[j + 1, z : z + 1, :] + coefs[j] * rate


def two_steps_kernel(first, m, edge_m, fp, lists, got_up, got_down, v_in, s_in, q_in, v, s, q, rates):
    up, down = (UP_FIRST, DOWN_FIRST) if first else (UP, DOWN)
    refs = (v, s, q, m)
    for i, (f, z) in enumerate(UP):
        plane_of(refs, f, z + 8)[...] = unpacked(got_up, up, i)
    for i, (f, z) in enumerate(DOWN):
        plane_of(refs, f, z - 8)[...] = unpacked(got_down, down, i)
    sxz, syz, szz = SXZ - SXX, SYZ - SXX, SZZ - SXX
    for z in range(2, 10):
        for f in ALL_V:
            plane = v_in[f, z]
            if z == 2 and f == VX:
                plane = plane - m[0, 0] * s[sxz, 1]
            if z == 2 and f == VY:
                plane = plane - m[0, 0] * s[syz, 1]
            if z == 9 and f == VZ:
                plane = plane + m[0, 7] * s[szz, 10]
            v[f, z] = plane
    v[VX, 10] -= edge_m[0, 1] * s_in[sxz, 9]
    v[VY, 10] -= edge_m[0, 1] * s_in[syz, 9]
    v[VZ, 1] += edge_m[0, 0] * s_in[szz, 2]

    def stress(f, z):
        return q[z] if f == SXY else s[f - SXX, z]

    def stress_a(z, s_from, q_from, lam, mu, want):
        for f, change in stress_change(v, z, lam, mu, want).items():
            if f == SXY:
                q[z] = q_from[z] + change
            else:
                s[f - SXX, z] = s_from[f - SXX, z] + change
        if SXY in want:
            slide(q, fp, z, fp[0, pl.ds(z, 1), :] + FRIC * rate_at(v, z) - lists[0, pl.ds(z, 1), :])

    def velocity_b(z, b, want):
        for f, change in velocity_change(stress, z, b, want).items():
            v[f, z] += change

    def own_stress_a(z, carry):
        stress_a(z, s_in, q_in, m[1, z - 2], m[2, z - 2], ALL_S)
        return carry

    def own_velocity_b(z, carry):
        velocity_b(z, m[0, z - 2], ALL_V)
        return carry

    def own_stress_b(z, carry):
        for f, change in stress_change(v, z, m[1, z - 2], m[2, z - 2], ALL_S).items():
            if f == SXY:
                q[z] += change
            else:
                s[f - SXX, z] += change
        slide(q, fp, z, fp[0, pl.ds(z, 1), :] + FRIC * rate_at(v, z))
        return carry

    stress_a(1, s, q, edge_m[1, 0], edge_m[2, 0], (SZZ, SXZ, SYZ))
    lax.fori_loop(2, 10, own_stress_a, 0)
    stress_a(10, s, q, edge_m[1, 1], edge_m[2, 1], ALL_S)
    velocity_b(1, edge_m[0, 0], (VZ,))
    lax.fori_loop(2, 10, own_velocity_b, 0)
    velocity_b(10, edge_m[0, 1], (VX, VY))
    rates[...] = jnp.zeros_like(rates)
    for z in range(2, 11):
        rates[z : z + 1, :] = rate_at(v, z)
    lax.fori_loop(2, 10, own_stress_b, 0)
    empty = jnp.zeros((NY, EXT), jnp.float32)
    s[sxz, 1] = empty
    s[syz, 1] = empty
    s[szz, 10] = empty


def part_kernel(coefs, m, fp, lists, rates, s, v_in, q_in, v, q, sent, up, down):
    for j in range(lists.shape[0] - 1):
        sent[j] = lists[j + 1] + coefs[j] * rates[...]
    refs = (v, s, q, m)

    def step(z, carry):
        q[z] = q_in[z]
        slide(q, fp, z, q[z, Y0 : Y0 + 1, :] - lists[0, pl.ds(z, 1), :])
        for f, change in move_first(refs, z).items():
            v[f, z] = v_in[f, z] + change
        return carry

    lax.fori_loop(2, 10, step, 0)
    pack(refs, UP, up)
    pack(refs, DOWN, down)


def end_kernel(fp, lists, v, s, q, vel, str_):
    for z in range(8):
        for f in ALL_V:
            vel[f, z] = v[f, z + 2, :, :LANES]
        for i, f in enumerate((SXX, None, SXZ, SYZ, SZZ, SYY)):
            str_[i, z] = q[z + 2, :, :LANES] if f is None else s[f - SXX, z + 2, :, :LANES]
        row = q[z + 2, Y0 : Y0 + 1, :LANES]
        slides = fp[1, z + 2 : z + 3, :LANES] > 0.5
        str_[1, z, Y0 : Y0 + 1, :] = jnp.where(slides, row - lists[0, z + 2 : z + 3, :LANES], row)


def along_strike(value, by):
    n = lax.axis_size("strike")
    return lax.ppermute(value, "strike", [(i, (i + by) % n) for i in range(n)])


def along_depth(value, by):
    n = lax.axis_size("depth")
    return lax.ppermute(value, "depth", [(i, i + by) for i in range(n) if 0 <= i + by < n])


def per_device(velocity, stress, b, lam, mu, past, coefs, pre, fault_mask):
    mask = fault_mask.astype(jnp.float32)
    edge = (7, NY, LANES)
    to_next, to_prev, owed = call(
        edges_kernel, [edge, edge, (STEPS, 8, LANES)], [coefs, past, velocity, stress, b, lam, mu, pre, mask], smem=(0,)
    )
    from_prev = along_strike(to_next, 1)
    from_next = along_strike(to_prev, -1)
    v3, s5, q1, m3 = (3, 12, NY, EXT), (5, 12, NY, EXT), (12, NY, EXT), (3, 8, NY, EXT)
    edge, plane = (3, 2, NY, EXT), (ROWS, EXT)
    v, s, q, m, fp, lists, up, down = call(
        start_kernel,
        [v3, s5, q1, m3, (2, *plane), (STEPS, *plane), (tiles(UP_FIRST) + 1, NY, LANES), (tiles(DOWN_FIRST), NY, LANES)],
        [velocity, stress, b, lam, mu, pre, mask, owed, from_prev, from_next],
    )
    edge_m = m
    for step in range(0, STEPS, 2):
        first = step == 0
        got_up = along_depth(up, -1)
        got_down = along_depth(down, 1)
        left = STEPS - step - 1
        more = call(
            functools.partial(meet_kernel, first),
            [(left, *plane)] + ([edge, (2, *plane), (STEPS, *plane)] if first else []),
            [coefs, got_up, got_down, v, s, m, edge_m, fp, lists],
            smem=(0,),
        )
        if first:
            edge_m, fp, lists = more[1:]
        got = along_strike(more[0], 1)
        v, s, q, rates = call(
            functools.partial(two_steps_kernel, first),
            [v3, s5, q1, plane],
            [m, edge_m, fp, lists, got_up, got_down, v, s, q],
            {6: 0, 7: 1, 8: 2},
        )
        if step + 2 < STEPS:
            v, q, sent, up, down = call(
                part_kernel,
                [v3, q1, (left - 1, *plane), (tiles(UP), NY, LANES), (tiles(DOWN), NY, LANES)],
                [coefs, m, fp, got, rates, s, v, q],
                {6: 0, 7: 1},
                smem=(0,),
            )
            lists = along_strike(sent, 1)
    return tuple(call(end_kernel, [velocity.shape, stress.shape], [fp, got, v, s, q]))


def solution(mesh):
    placed = (
        P(None, "depth", None, "strike"),
        P(None, "depth", None, "strike"),
        P("depth", None, "strike"),
        P("depth", None, "strike"),
        P("depth", None, "strike"),
        P(None, "depth", "strike"),
        P(),
        P("depth", "strike"),
        P("depth", "strike"),
    )
    return jax.shard_map(
        per_device,
        mesh=mesh,
        in_specs=placed,
        out_specs=(P(None, "depth", None, "strike"), P(None, "depth", None, "strike")),
        check_vma=False,
    )
```

```python
import functools

import jax
import jax.numpy as jnp
from jax import lax
from jax.experimental import pallas as pl
from jax.experimental.pallas import tpu as pltpu
from jax.sharding import PartitionSpec as P


HIST = 64
STEPS = 8
DT = 0.3
FRIC = 0.5

NY = 32
Y0 = NY // 2
LANES = 128
EXT = 2 * LANES
W = STEPS
ROWS = 16
VMEM = pl.BlockSpec(memory_space=pltpu.VMEM)
SMEM = pl.BlockSpec(memory_space=pltpu.SMEM)

VX, VY, VZ, SXX, SXZ, SYZ, SZZ, SYY, SXY, B, LAM, MU = range(12)

UP = ((VX, 2), (VX, 3), (VY, 2), (VY, 3), (VZ, 2), (SXX, 2), (SXZ, 2), (SYZ, 2), (SZZ, 2), (SYY, 2), (SXY, 2))
DOWN = ((VX, 9), (VY, 9), (VZ, 8), (VZ, 9), (SXZ, 9), (SYZ, 9), (SZZ, 9))
UP_FIRST = UP + ((B, 2), (LAM, 2), (MU, 2))
DOWN_FIRST = DOWN + ((B, 9), (LAM, 9), (MU, 9))


def tiles(planes):
    return len(planes) + -(-len(planes) // 8)


def call(body, outs, ins, aliases=None, smem=()):
    return pl.pallas_call(
        body,
        out_shape=[jax.ShapeDtypeStruct(s, jnp.float32) for s in outs],
        in_specs=[SMEM if i in smem else VMEM for i in range(len(ins))],
        out_specs=[VMEM] * len(outs),
        input_output_aliases=aliases or {},
        compiler_params=pltpu.CompilerParams(vmem_limit_bytes=32 * 1024 * 1024),
        cost_estimate=pl.CostEstimate(flops=4_000_000, bytes_accessed=4_000_000, transcendentals=0),
    )(*ins)


def lane_of(rows):
    return lax.broadcasted_iota(jnp.int32, (rows, LANES), 1)


def rolled(tile, by):
    by %= LANES
    return tile if by == 0 else pltpu.roll(tile, by, 1)


def ahead_x(f):
    return pltpu.roll(f, f.shape[1] - 1, 1)


def behind_x(f):
    return pltpu.roll(f, 1, 1)


def ahead_y(f):
    row = lax.broadcasted_iota(jnp.int32, f.shape, 0)
    return jnp.where(row == NY - 1, 0.0, pltpu.roll(f, NY - 1, 0))


def behind_y(f):
    row = lax.broadcasted_iota(jnp.int32, f.shape, 0)
    return jnp.where(row == 0, 0.0, pltpu.roll(f, 1, 0))


def plane_of(refs, f, z):
    v, s, q, m = refs
    if f < SXX:
        return v.at[f, z]
    if f < SXY:
        return s.at[f - SXX, z]
    if f == SXY:
        return q.at[z]
    return m.at[f - B, z - 2]


def velocity_change(stress, z, b, want):
    sxy, sxz, syz, szz = stress(SXY, z), stress(SXZ, z), stress(SYZ, z), stress(SZZ, z)
    out = {}
    if VX in want:
        sxx = stress(SXX, z)
        out[VX] = b * ((ahead_x(sxx) - sxx) + (sxy - behind_y(sxy)) + (sxz - stress(SXZ, z - 1)))
    if VY in want:
        syy = stress(SYY, z)
        out[VY] = b * ((sxy - behind_x(sxy)) + (ahead_y(syy) - syy) + (syz - stress(SYZ, z - 1)))
    if VZ in want:
        out[VZ] = b * ((sxz - behind_x(sxz)) + (syz - behind_y(syz)) + (stress(SZZ, z + 1) - szz))
    return out


def stress_change(v, z, lam, mu, want):
    vx, vy, vz = v[VX, z], v[VY, z], v[VZ, z]
    ex = vx - behind_x(vx)
    ey = vy - behind_y(vy)
    ez = vz - v[VZ, z - 1]
    spread = lam * (ex + ey + ez)
    twice = mu + mu
    out = {}
    if SXX in want:
        out[SXX] = spread + twice * ex
        out[SYY] = spread + twice * ey
        out[SXY] = mu * ((ahead_y(vx) - vx) + (ahead_x(vy) - vy))
    out[SZZ] = spread + twice * ez
    out[SXZ] = mu * ((v[VX, z + 1] - vx) + (ahead_x(vz) - vz))
    out[SYZ] = mu * ((v[VY, z + 1] - vy) + (ahead_y(vz) - vz))
    return out


ALL_V = (VX, VY, VZ)
ALL_S = (SXX, SXZ, SYZ, SZZ, SYY, SXY)


def rate_at(v, z):
    return v[VX, z, Y0 + 1 : Y0 + 2, :] - v[VX, z, Y0 : Y0 + 1, :]


def slide(q, fp, z, traction):
    slides = fp[1, pl.ds(z, 1), :] > 0.5
    q[z, Y0 : Y0 + 1, :] = jnp.where(slides, traction, q[z, Y0 : Y0 + 1, :])


def pack(refs, planes, out):
    lane = lane_of(NY)
    for first in range(0, len(planes), 8):
        edges = jnp.zeros((NY, LANES), jnp.float32)
        for i, (f, z) in enumerate(planes[first : first + 8]):
            ref = plane_of(refs, f, z)
            out[first + i] = ref[:, :LANES]
            moved = rolled(ref[:, LANES:], W + 2 * W * i)
            edges = jnp.where((lane >= 2 * W * i) & (lane < 2 * W * (i + 1)), moved, edges)
        out[len(planes) + first // 8] = edges


def unpacked(got, planes, i, rows=slice(None)):
    edges = got[len(planes) + i // 8, rows, :]
    return jnp.concatenate([got[i, rows, :], rolled(edges, -(W + 2 * W * (i % 8)))], axis=1)


def owed_kernel(coefs, past, owed):
    for j in range(STEPS):
        parts = [None] * 4
        for k in range(HIST - j):
            term = coefs[j + k] * past[k]
            parts[k % 4] = term if parts[k % 4] is None else parts[k % 4] + term
        owed[j] = (parts[0] + parts[1]) + (parts[2] + parts[3])


def edges_kernel(fields, pre, mask, owed, to_next, to_prev):
    lane8 = lane_of(8)
    nxt = jnp.zeros((8, LANES), jnp.float32)
    prv = jnp.zeros((8, LANES), jnp.float32)
    for i, plane in enumerate([owed[j] for j in range(STEPS)] + [pre[...], mask[...].astype(jnp.float32)]):
        here = (lane8 >= W * i) & (lane8 < W * (i + 1))
        nxt = jnp.where(here, rolled(plane, W * i - (LANES - W)), nxt)
        prv = jnp.where(here, rolled(plane, W * i), prv)
    to_next[6] = jnp.zeros((NY, LANES), jnp.float32)
    to_prev[6] = jnp.zeros((NY, LANES), jnp.float32)
    to_next[6, 0:8, :] = nxt
    to_prev[6, 0:8, :] = prv
    lane = lane_of(NY)
    for t in range(6):
        nxt = jnp.zeros((NY, LANES), jnp.float32)
        prv = jnp.zeros((NY, LANES), jnp.float32)
        for i in range(16):
            plane = fields[2 * t + i // 8, i % 8]
            here = (lane >= W * i) & (lane < W * (i + 1))
            nxt = jnp.where(here, rolled(plane, W * i - (LANES - W)), nxt)
            prv = jnp.where(here, rolled(plane, W * i), prv)
        to_next[t] = nxt
        to_prev[t] = prv


def move_first(refs, z, q_now=None):
    _, s, q, m = refs

    def stress(f, at):
        return (q if q_now is None else q_now)[at] if f == SXY else s[f - SXX, at]

    return velocity_change(stress, z, m[0, z - 2], ALL_V)


def start_kernel(fields, pre, mask, owed, from_prev, from_next, v, s, q, m, fp, lists, up, down):
    lane = lane_of(NY)
    lane8 = lane_of(8)
    empty = jnp.zeros((NY, EXT), jnp.float32)
    s[SXZ - SXX, 1] = empty
    s[SYZ - SXX, 1] = empty
    s[SZZ - SXX, 10] = empty
    refs = (v, s, q, m)
    for k, f in enumerate((VX, VY, VZ, SXX, SXY, SXZ, SYZ, SZZ, SYY, B, LAM, MU)):
        for z in range(8):
            at = (k % 2) * 8 + z
            edge = jnp.where(
                lane < LANES // 2,
                rolled(from_next[k // 2], -W * at),
                rolled(from_prev[k // 2], LANES - W - W * at),
            )
            to = plane_of(refs, f, z + 2)
            to[:, :LANES] = fields[k, z]
            to[:, LANES:] = edge
    fp[...] = jnp.zeros_like(fp)
    lists[...] = jnp.zeros_like(lists)
    for i in range(STEPS + 2):
        plane = owed[i] if i < STEPS else (pre, mask)[i - STEPS][...].astype(jnp.float32)
        edge = jnp.where(
            lane8 < LANES // 2,
            rolled(from_next[6, 0:8, :], -W * i),
            rolled(from_prev[6, 0:8, :], LANES - W - W * i),
        )
        to, j = (lists, i) if i < STEPS else (fp, i - STEPS)
        to[j, 2:10, :LANES] = plane
        to[j, 2:10, LANES:] = edge

    def step(z, carry):
        for f, change in move_first(refs, z).items():
            v[f, z] += change
        return carry

    lax.fori_loop(2, 10, step, 0, unroll=4)
    pack(refs, UP_FIRST, up)
    pack(refs, DOWN_FIRST, down)
    last = tiles(UP_FIRST)
    up[last] = jnp.zeros((NY, LANES), jnp.float32)
    for i in range(STEPS + 2):
        to, j = (lists, i) if i < STEPS else (fp, i - STEPS)
        up[last, i : i + 1, :] = to[j, 2:3, :LANES]
        up[last, 16 + i : 17 + i, :] = to[j, 2:3, LANES:]


def meet_kernel(first, coefs, got_up, got_down, v, s, m, edge_m, fp, lists, sent, *more):
    up, down = (UP_FIRST, DOWN_FIRST) if first else (UP, DOWN)
    if first:
        edge_out, fp_out, lists_out = more
        for k in range(3):
            edge_out[k, 0] = unpacked(got_down, down, down.index((B + k, 9)))
            edge_out[k, 1] = unpacked(got_up, up, up.index((B + k, 2)))
        fp_out[...] = fp[...]
        lists_out[...] = lists[...]
        last = tiles(up)
        for i in range(STEPS + 2):
            to, j = (lists_out, i) if i < STEPS else (fp_out, i - STEPS)
            to[j, 10:11, :LANES] = got_up[last, i : i + 1, :]
            to[j, 10:11, LANES:] = got_up[last, 16 + i : 17 + i, :]
        edge_m, lists = edge_out, lists_out
    rows = slice(Y0, Y0 + 8)
    for z in range(2, 11):
        if z < 10:
            vx = v[VX, z, rows, :]
        else:
            vx = unpacked(got_up, up, up.index((VX, 2)), rows) - edge_m[0, 1, rows, :] * s[SXZ - SXX, 9, rows, :]
        if z == 2:
            vx = vx - m[0, 0, rows, :] * unpacked(got_down, down, down.index((SXZ, 9)), rows)
        rate = vx[1:2, :] - vx[0:1, :]
        for j in range(lists.shape[0] - 1):
            sent[j, z : z + 1, :] = lists[j + 1, z : z + 1, :] + coefs[j] * rate


def two_steps_kernel(first, m, edge_m, fp, lists, got_up, got_down, v_in, s_in, q_in, v, s, q, rates):
    up, down = (UP_FIRST, DOWN_FIRST) if first else (UP, DOWN)
    refs = (v, s, q, m)
    for i, (f, z) in enumerate(UP):
        plane_of(refs, f, z + 8)[...] = unpacked(got_up, up, i)
    for i, (f, z) in enumerate(DOWN):
        plane_of(refs, f, z - 8)[...] = unpacked(got_down, down, i)
    sxz, syz, szz = SXZ - SXX, SYZ - SXX, SZZ - SXX
    for z in range(2, 10):
        for f in ALL_V:
            plane = v_in[f, z]
            if z == 2 and f == VX:
                plane = plane - m[0, 0] * s[sxz, 1]
            if z == 2 and f == VY:
                plane = plane - m[0, 0] * s[syz, 1]
            if z == 9 and f == VZ:
                plane = plane + m[0, 7] * s[szz, 10]
            v[f, z] = plane
    v[VX, 10] -= edge_m[0, 1] * s_in[sxz, 9]
    v[VY, 10] -= edge_m[0, 1] * s_in[syz, 9]
    v[VZ, 1] += edge_m[0, 0] * s_in[szz, 2]

    def stress(f, z):
        return q[z] if f == SXY else s[f - SXX, z]

    def stress_a(z, s_from, q_from, lam, mu, want):
        for f, change in stress_change(v, z, lam, mu, want).items():
            if f == SXY:
                q[z] = q_from[z] + change
            else:
                s[f - SXX, z] = s_from[f - SXX, z] + change
        if SXY in want:
            slide(q, fp, z, fp[0, pl.ds(z, 1), :] + FRIC * rate_at(v, z) - lists[0, pl.ds(z, 1), :])

    def velocity_b(z, b, want):
        for f, change in velocity_change(stress, z, b, want).items():
            v[f, z] += change

    def own_stress_a(z, carry):
        stress_a(z, s_in, q_in, m[1, z - 2], m[2, z - 2], ALL_S)
        return carry

    def own_velocity_b(z, carry):
        velocity_b(z, m[0, z - 2], ALL_V)
        return carry

    def own_stress_b(z, carry):
        for f, change in stress_change(v, z, m[1, z - 2], m[2, z - 2], ALL_S).items():
            if f == SXY:
                q[z] += change
            else:
                s[f - SXX, z] += change
        slide(q, fp, z, fp[0, pl.ds(z, 1), :] + FRIC * rate_at(v, z))
        return carry

    stress_a(1, s, q, edge_m[1, 0], edge_m[2, 0], (SZZ, SXZ, SYZ))
    lax.fori_loop(2, 10, own_stress_a, 0, unroll=4)
    stress_a(10, s, q, edge_m[1, 1], edge_m[2, 1], ALL_S)
    velocity_b(1, edge_m[0, 0], (VZ,))
    lax.fori_loop(2, 10, own_velocity_b, 0, unroll=4)
    velocity_b(10, edge_m[0, 1], (VX, VY))
    rates[...] = jnp.zeros_like(rates)
    for z in range(2, 11):
        rates[z : z + 1, :] = rate_at(v, z)
    lax.fori_loop(2, 10, own_stress_b, 0, unroll=4)
    empty = jnp.zeros((NY, EXT), jnp.float32)
    s[sxz, 1] = empty
    s[syz, 1] = empty
    s[szz, 10] = empty


def part_kernel(m, fp, lists, s, v_in, q_in, v, q, up, down):
    refs = (v, s, q, m)

    def step(z, carry):
        q[z] = q_in[z]
        slide(q, fp, z, q[z, Y0 : Y0 + 1, :] - lists[0, pl.ds(z, 1), :])
        for f, change in move_first(refs, z).items():
            v[f, z] = v_in[f, z] + change
        return carry

    lax.fori_loop(2, 10, step, 0, unroll=4)
    pack(refs, UP, up)
    pack(refs, DOWN, down)


def end_kernel(fp, lists, v, s, q, vel, str_):
    for z in range(8):
        for f in ALL_V:
            vel[f, z] = v[f, z + 2, :, :LANES]
        for i, f in enumerate((SXX, None, SXZ, SYZ, SZZ, SYY)):
            str_[i, z] = q[z + 2, :, :LANES] if f is None else s[f - SXX, z + 2, :, :LANES]
        row = q[z + 2, Y0 : Y0 + 1, :LANES]
        slides = fp[1, z + 2 : z + 3, :LANES] > 0.5
        str_[1, z, Y0 : Y0 + 1, :] = jnp.where(slides, row - lists[0, z + 2 : z + 3, :LANES], row)


def along_strike(value, by):
    n = lax.axis_size("strike")
    return lax.ppermute(value, "strike", [(i, (i + by) % n) for i in range(n)])


def along_depth(value, by):
    n = lax.axis_size("depth")
    return lax.ppermute(value, "depth", [(i, i + by) for i in range(n) if 0 <= i + by < n])


def per_device(velocity, stress, b, lam, mu, past, coefs, pre, mask):
    edge = (7, NY, LANES)
    (owed,) = call(owed_kernel, [(STEPS, 8, LANES)], [coefs, past], smem=(0,))
    fields = jnp.concatenate([velocity, stress, DT * b[None], DT * lam[None], DT * mu[None]])
    to_next, to_prev = call(edges_kernel, [edge, edge], [fields, pre, mask, owed])
    from_prev = along_strike(to_next, 1)
    from_next = along_strike(to_prev, -1)
    v3, s5, q1, m3 = (3, 12, NY, EXT), (5, 12, NY, EXT), (12, NY, EXT), (3, 8, NY, EXT)
    edge, plane = (3, 2, NY, EXT), (ROWS, EXT)
    v, s, q, m, fp, lists, up, down = call(
        start_kernel,
        [v3, s5, q1, m3, (2, *plane), (STEPS, *plane), (tiles(UP_FIRST) + 1, NY, LANES), (tiles(DOWN_FIRST), NY, LANES)],
        [fields, pre, mask, owed, from_prev, from_next],
    )
    edge_m = m
    for step in range(0, STEPS, 2):
        first = step == 0
        got_up = along_depth(up, -1)
        got_down = along_depth(down, 1)
        left = STEPS - step - 1
        more = call(
            functools.partial(meet_kernel, first),
            [(left, *plane)] + ([edge, (2, *plane), (STEPS, *plane)] if first else []),
            [coefs, got_up, got_down, v, s, m, edge_m, fp, lists],
            smem=(0,),
        )
        if first:
            edge_m, fp, lists = more[1:]
        got = along_strike(more[0], 1)
        v, s, q, rates = call(
            functools.partial(two_steps_kernel, first),
            [v3, s5, q1, plane],
            [m, edge_m, fp, lists, got_up, got_down, v, s, q],
            {6: 0, 7: 1, 8: 2},
        )
        if step + 2 < STEPS:
            lists = along_strike(got[1:] + coefs[: left - 1, None, None] * rates[None], 1)
            v, q, up, down = call(
                part_kernel,
                [v3, q1, (tiles(UP), NY, LANES), (tiles(DOWN), NY, LANES)],
                [m, fp, got, s, v, q],
                {4: 0, 5: 1},
            )
    return tuple(call(end_kernel, [velocity.shape, stress.shape], [fp, got, v, s, q]))


def solution(mesh):
    placed = (
        P(None, "depth", None, "strike"),
        P(None, "depth", None, "strike"),
        P("depth", None, "strike"),
        P("depth", None, "strike"),
        P("depth", None, "strike"),
        P(None, "depth", "strike"),
        P(),
        P("depth", "strike"),
        P("depth", "strike"),
    )
    return jax.shard_map(
        per_device,
        mesh=mesh,
        in_specs=placed,
        out_specs=(P(None, "depth", None, "strike"), P(None, "depth", None, "strike")),
        check_vma=False,
    )
```

```python
import functools

import jax
import jax.numpy as jnp
from jax import lax
from jax.experimental import pallas as pl
from jax.experimental.pallas import tpu as pltpu
from jax.sharding import PartitionSpec as P


HIST = 64
STEPS = 8
DT = 0.3
FRIC = 0.5

NY = 32
Y0 = NY // 2
LANES = 128
EXT = 2 * LANES
W = STEPS
ROWS = 16
VMEM = pl.BlockSpec(memory_space=pltpu.VMEM)
SMEM = pl.BlockSpec(memory_space=pltpu.SMEM)

VX, VY, VZ, SXX, SXZ, SYZ, SZZ, SYY, SXY, B, LAM, MU = range(12)

TRACES = 6
TILES = TRACES + 1
FIRST = TRACES + 3
FIRST_TILES = FIRST + 3


def call(body, outs, ins, aliases=None, smem=(), scratch=()):
    return pl.pallas_call(
        body,
        out_shape=[jax.ShapeDtypeStruct(s, jnp.float32) for s in outs],
        in_specs=[SMEM if i in smem else VMEM for i in range(len(ins))],
        out_specs=[VMEM] * len(outs),
        scratch_shapes=scratch,
        input_output_aliases=aliases or {},
        compiler_params=pltpu.CompilerParams(vmem_limit_bytes=32 * 1024 * 1024),
        cost_estimate=pl.CostEstimate(flops=4_000_000, bytes_accessed=4_000_000, transcendentals=0),
    )(*ins)


def lane_of(rows):
    return lax.broadcasted_iota(jnp.int32, (rows, LANES), 1)


def rolled(tile, by):
    by %= LANES
    return tile if by == 0 else pltpu.roll(tile, by, 1)


def ahead_x(f):
    return pltpu.roll(f, f.shape[1] - 1, 1)


def behind_x(f):
    return pltpu.roll(f, 1, 1)


def ahead_y(f):
    row = lax.broadcasted_iota(jnp.int32, f.shape, 0)
    return jnp.where(row == NY - 1, 0.0, pltpu.roll(f, NY - 1, 0))


def behind_y(f):
    row = lax.broadcasted_iota(jnp.int32, f.shape, 0)
    return jnp.where(row == 0, 0.0, pltpu.roll(f, 1, 0))


def plane_of(refs, f, z):
    v, s, q, m = refs
    if f < SXX:
        return v.at[f, z]
    if f < SXY:
        return s.at[f - SXX, z]
    if f == SXY:
        return q.at[z]
    return m.at[f - B, z - 2]


def velocity_change(stress, z, b, want):
    sxy, sxz, syz, szz = stress(SXY, z), stress(SXZ, z), stress(SYZ, z), stress(SZZ, z)
    out = {}
    if VX in want:
        sxx = stress(SXX, z)
        out[VX] = b * ((ahead_x(sxx) - sxx) + (sxy - behind_y(sxy)) + (sxz - stress(SXZ, z - 1)))
    if VY in want:
        syy = stress(SYY, z)
        out[VY] = b * ((sxy - behind_x(sxy)) + (ahead_y(syy) - syy) + (syz - stress(SYZ, z - 1)))
    if VZ in want:
        out[VZ] = b * ((sxz - behind_x(sxz)) + (syz - behind_y(syz)) + (stress(SZZ, z + 1) - szz))
    return out


def stress_change(velocity, z, lam, mu, want):
    vx, vy, vz = velocity(VX, z), velocity(VY, z), velocity(VZ, z)
    ex = vx - behind_x(vx)
    ey = vy - behind_y(vy)
    ez = vz - velocity(VZ, z - 1)
    spread = lam * (ex + ey + ez)
    twice = mu + mu
    out = {}
    if SXX in want:
        out[SXX] = spread + twice * ex
        out[SYY] = spread + twice * ey
        out[SXY] = mu * ((ahead_y(vx) - vx) + (ahead_x(vy) - vy))
    out[SZZ] = spread + twice * ez
    out[SXZ] = mu * ((velocity(VX, z + 1) - vx) + (ahead_x(vz) - vz))
    out[SYZ] = mu * ((velocity(VY, z + 1) - vy) + (ahead_y(vz) - vz))
    return out


ALL_V = (VX, VY, VZ)
ALL_S = (SXX, SXZ, SYZ, SZZ, SYY, SXY)


def rate_at(v, z):
    return v[VX, z, Y0 + 1 : Y0 + 2, :] - v[VX, z, Y0 : Y0 + 1, :]


def slide(q, fp, z, traction):
    slides = fp[1, pl.ds(z, 1), :] > 0.5
    q[z, Y0 : Y0 + 1, :] = jnp.where(slides, traction, q[z, Y0 : Y0 + 1, :])


def slid(plane, fp, z, traction):
    row = lax.broadcasted_iota(jnp.int32, plane.shape, 0)
    return jnp.where((row == Y0) & (fp[1, z : z + 1, :] > 0.5), traction, plane)


def packed(planes):
    lane = lane_of(NY)
    out = [plane[:, :LANES] for plane in planes]
    for first in range(0, len(planes), 8):
        edges = jnp.zeros((NY, LANES), jnp.float32)
        for i, plane in enumerate(planes[first : first + 8]):
            moved = rolled(plane[:, LANES:], W + 2 * W * i)
            edges = jnp.where((lane >= 2 * W * i) & (lane < 2 * W * (i + 1)), moved, edges)
        out.append(edges)
    return out


def even_depth():
    return lax.axis_index("depth") % 2 == 0


def post(up, down, one, two):
    even = even_depth()
    for i, (u, d) in enumerate(zip(up, down, strict=True)):
        one[i] = jnp.where(even, d, u)
        two[i] = jnp.where(even, u, d)


class Got:
    def __init__(self, one, two, count):
        self.one, self.two, self.count, self.even = one, two, count, even_depth()

    def tile(self, above, i, rows):
        first, second = (self.one, self.two) if above else (self.two, self.one)
        return jnp.where(self.even, first[i, rows, :], second[i, rows, :])

    def plane(self, above, i, rows=slice(None)):
        edges = self.tile(above, self.count + i // 8, rows)
        return jnp.concatenate([self.tile(above, i, rows), rolled(edges, -(W + 2 * W * (i % 8)))], axis=1)


def traces(refs, fp):
    v, s, q, m = refs
    nothing = jnp.zeros((NY, EXT), jnp.float32)

    def alone(f, z):
        return v[f, z] if 2 <= z < 10 else nothing

    def before(f, z):
        return q[z] if f == SXY else s[f - SXX, z]

    def carried(z, want_s, want_v):
        now = {f: before(f, z) + c for f, c in stress_change(alone, z, m[1, z - 2], m[2, z - 2], want_s).items()}
        if SXY in now:
            now[SXY] = slid(now[SXY], fp, z, fp[0, z : z + 1, :] + FRIC * rate_at(v, z))
        change = velocity_change(lambda f, at: now.get(f, nothing) if at == z else nothing, z, m[0, z - 2], want_v)
        return now, {f: v[f, z] + c for f, c in change.items()}

    now, then = carried(2, ALL_S, (VX, VY))
    up = [v[VX, 2], v[VY, 2], before(SZZ, 2), now[SZZ], then[VX], then[VY]]
    now, then = carried(9, (SZZ, SXZ, SYZ), (VZ,))
    down = [before(SXZ, 9), before(SYZ, 9), v[VZ, 9], now[SXZ], now[SYZ], then[VZ]]
    return up, down


def owed_kernel(coefs, past, owed):
    for j in range(STEPS):
        parts = [None] * 4
        for k in range(HIST - j):
            term = coefs[j + k] * past[k]
            parts[k % 4] = term if parts[k % 4] is None else parts[k % 4] + term
        owed[j] = (parts[0] + parts[1]) + (parts[2] + parts[3])


def edges_kernel(fields, pre, mask, owed, to_next, to_prev):
    lane8 = lane_of(8)
    nxt = jnp.zeros((8, LANES), jnp.float32)
    prv = jnp.zeros((8, LANES), jnp.float32)
    for i, plane in enumerate([owed[j] for j in range(STEPS)] + [pre[...], mask[...].astype(jnp.float32)]):
        here = (lane8 >= W * i) & (lane8 < W * (i + 1))
        nxt = jnp.where(here, rolled(plane, W * i - (LANES - W)), nxt)
        prv = jnp.where(here, rolled(plane, W * i), prv)
    to_next[6] = jnp.zeros((NY, LANES), jnp.float32)
    to_prev[6] = jnp.zeros((NY, LANES), jnp.float32)
    to_next[6, 0:8, :] = nxt
    to_prev[6, 0:8, :] = prv
    lane = lane_of(NY)
    for t in range(6):
        nxt = jnp.zeros((NY, LANES), jnp.float32)
        prv = jnp.zeros((NY, LANES), jnp.float32)
        for i in range(16):
            plane = fields[2 * t + i // 8, i % 8]
            here = (lane >= W * i) & (lane < W * (i + 1))
            nxt = jnp.where(here, rolled(plane, W * i - (LANES - W)), nxt)
            prv = jnp.where(here, rolled(plane, W * i), prv)
        to_next[t] = nxt
        to_prev[t] = prv


def move_first(refs, z, q_now=None):
    _, s, q, m = refs

    def stress(f, at):
        return (q if q_now is None else q_now)[at] if f == SXY else s[f - SXX, at]

    return velocity_change(stress, z, m[0, z - 2], ALL_V)


def start_kernel(fields, pre, mask, owed, from_prev, from_next, v, s, q, m, fp, lists, one, two):
    lane = lane_of(NY)
    lane8 = lane_of(8)
    empty = jnp.zeros((NY, EXT), jnp.float32)
    s[SXZ - SXX, 1] = empty
    s[SYZ - SXX, 1] = empty
    s[SZZ - SXX, 10] = empty
    refs = (v, s, q, m)
    for k, f in enumerate((VX, VY, VZ, SXX, SXY, SXZ, SYZ, SZZ, SYY, B, LAM, MU)):
        for z in range(8):
            at = (k % 2) * 8 + z
            edge = jnp.where(
                lane < LANES // 2,
                rolled(from_next[k // 2], -W * at),
                rolled(from_prev[k // 2], LANES - W - W * at),
            )
            to = plane_of(refs, f, z + 2)
            to[:, :LANES] = fields[k, z]
            to[:, LANES:] = edge
    fp[...] = jnp.zeros_like(fp)
    lists[...] = jnp.zeros_like(lists)
    for i in range(STEPS + 2):
        plane = owed[i] if i < STEPS else (pre, mask)[i - STEPS][...].astype(jnp.float32)
        edge = jnp.where(
            lane8 < LANES // 2,
            rolled(from_next[6, 0:8, :], -W * i),
            rolled(from_prev[6, 0:8, :], LANES - W - W * i),
        )
        to, j = (lists, i) if i < STEPS else (fp, i - STEPS)
        to[j, 2:10, :LANES] = plane
        to[j, 2:10, LANES:] = edge

    def step(z, carry):
        for f, change in move_first(refs, z).items():
            v[f, z] += change
        return carry

    lax.fori_loop(2, 10, step, 0, unroll=4)
    up, down = traces(refs, fp)
    up = packed(up + [m[k, 0] for k in range(3)])
    down = packed(down + [m[k, 7] for k in range(3)])
    post(up, down, one, two)
    last = len(up)
    one[last] = jnp.zeros((NY, LANES), jnp.float32)
    two[last] = jnp.zeros((NY, LANES), jnp.float32)
    for i in range(STEPS + 2):
        to, j = (lists, i) if i < STEPS else (fp, i - STEPS)
        for out in (one, two):
            out[last, i : i + 1, :] = to[j, 2:3, :LANES]
            out[last, 16 + i : 17 + i, :] = to[j, 2:3, LANES:]


def meet_kernel(first, coefs, one, two, v, s, m, edge_m, fp, lists, sent, *more):
    *more, rates = more
    got = Got(one, two, FIRST if first else TRACES)
    if first:
        edge_out, fp_out, lists_out = more
        for k in range(3):
            edge_out[k, 0] = got.plane(False, TRACES + k)
            edge_out[k, 1] = got.plane(True, TRACES + k)
        fp_out[...] = fp[...]
        lists_out[...] = lists[...]
        for i in range(STEPS + 2):
            to, j = (lists_out, i) if i < STEPS else (fp_out, i - STEPS)
            to[j, 10:11, :LANES] = got.tile(True, FIRST_TILES - 1, slice(i, i + 1))
            to[j, 10:11, LANES:] = got.tile(True, FIRST_TILES - 1, slice(16 + i, 17 + i))
        edge_m, lists = edge_out, lists_out
    rows = slice(Y0, Y0 + 8)
    rates[...] = jnp.zeros_like(rates)
    for z in range(2, 11):
        if z < 10:
            vx = v[VX, z, rows, :]
        else:
            vx = got.plane(True, 0, rows) - edge_m[0, 1, rows, :] * s[SXZ - SXX, 9, rows, :]
        if z == 2:
            vx = vx - m[0, 0, rows, :] * got.plane(False, 0, rows)
        rates[z : z + 1, :] = vx[1:2, :] - vx[0:1, :]
    for j in range(lists.shape[0] - 1):
        sent[j] = lists[j + 1] + coefs[j] * rates[...]


def two_steps_kernel(first, m, edge_m, fp, lists, one, two, v_in, s_in, q_in, v, s, q, rates):
    got = Got(one, two, FIRST if first else TRACES)
    sxz, syz, szz = SXZ - SXX, SYZ - SXX, SZZ - SXX
    nothing = jnp.zeros((NY, EXT), jnp.float32)
    for z in range(2, 10):
        for f in ALL_V:
            plane = v_in[f, z]
            if z == 2 and f == VX:
                plane = plane - m[0, 0] * got.plane(False, 0)
            if z == 2 and f == VY:
                plane = plane - m[0, 0] * got.plane(False, 1)
            if z == 9 and f == VZ:
                plane = plane + m[0, 7] * got.plane(True, 2)
            v[f, z] = plane
    above = {VX: -(edge_m[0, 1] * s_in[sxz, 9]), VY: -(edge_m[0, 1] * s_in[syz, 9])}
    below = {VZ: edge_m[0, 0] * s_in[szz, 2]}
    v[VX, 10] = got.plane(True, 0) + above[VX]
    v[VY, 10] = got.plane(True, 1) + above[VY]
    v[VZ, 1] = got.plane(False, 2) + below[VZ]
    more_above = stress_change(
        lambda f, z: above.get(f, nothing) if z == 10 else v[f, z] if z == 9 else nothing,
        10,
        edge_m[1, 1],
        edge_m[2, 1],
        ALL_S,
    )
    slip = above[VX][Y0 + 1 : Y0 + 2, :] - above[VX][Y0 : Y0 + 1, :]
    more_above[SXY] = slid(more_above[SXY], fp, 10, FRIC * slip - lists[0, 10:11, :])
    more_below = stress_change(
        lambda f, z: below.get(f, nothing) if z == 1 else v[f, z] if z == 2 else nothing,
        1,
        edge_m[1, 0],
        edge_m[2, 0],
        (SZZ, SXZ, SYZ),
    )
    s[szz, 10] = got.plane(True, 3) + more_above[SZZ]
    s[sxz, 1] = got.plane(False, 3) + more_below[SXZ]
    s[syz, 1] = got.plane(False, 4) + more_below[SYZ]

    def velocity(f, z):
        return v[f, z]

    def stress(f, z):
        return q[z] if f == SXY else s[f - SXX, z]

    def own_stress_a(z, carry):
        for f, change in stress_change(velocity, z, m[1, z - 2], m[2, z - 2], ALL_S).items():
            if f == SXY:
                q[z] = q_in[z] + change
            else:
                s[f - SXX, z] = s_in[f - SXX, z] + change
        slide(q, fp, z, fp[0, pl.ds(z, 1), :] + FRIC * rate_at(v, z) - lists[0, pl.ds(z, 1), :])
        return carry

    def own_velocity_b(z, carry):
        for f, change in velocity_change(stress, z, m[0, z - 2], ALL_V).items():
            v[f, z] += change
        return carry

    def own_stress_b(z, carry):
        for f, change in stress_change(velocity, z, m[1, z - 2], m[2, z - 2], ALL_S).items():
            if f == SXY:
                q[z] += change
            else:
                s[f - SXX, z] += change
        slide(q, fp, z, fp[0, pl.ds(z, 1), :] + FRIC * rate_at(v, z))
        return carry

    lax.fori_loop(2, 10, own_stress_a, 0, unroll=4)
    change = velocity_change(
        lambda f, z: more_above[f] if z == 10 else s[f - SXX, 9], 10, edge_m[0, 1], (VX, VY)
    )
    v[VX, 10] = got.plane(True, 4) + above[VX] + change[VX]
    v[VY, 10] = got.plane(True, 5) + above[VY] + change[VY]
    change = velocity_change(
        lambda f, z: more_below.get(f, nothing) if z == 1 else s[f - SXX, 2], 1, edge_m[0, 0], (VZ,)
    )
    v[VZ, 1] = got.plane(False, 5) + below[VZ] + change[VZ]
    lax.fori_loop(2, 10, own_velocity_b, 0, unroll=4)
    rates[...] = jnp.zeros_like(rates)
    for z in range(2, 11):
        rates[z : z + 1, :] = rate_at(v, z)
    lax.fori_loop(2, 10, own_stress_b, 0, unroll=4)
    s[sxz, 1] = nothing
    s[syz, 1] = nothing
    s[szz, 10] = nothing


def part_kernel(m, fp, lists, s, v_in, q_in, v, q, one, two):
    refs = (v, s, q, m)

    def step(z, carry):
        q[z] = q_in[z]
        slide(q, fp, z, q[z, Y0 : Y0 + 1, :] - lists[0, pl.ds(z, 1), :])
        for f, change in move_first(refs, z).items():
            v[f, z] = v_in[f, z] + change
        return carry

    lax.fori_loop(2, 10, step, 0, unroll=4)
    up, down = traces(refs, fp)
    post(packed(up), packed(down), one, two)


def end_kernel(fp, lists, v, s, q, vel, str_):
    for z in range(8):
        for f in ALL_V:
            vel[f, z] = v[f, z + 2, :, :LANES]
        for i, f in enumerate((SXX, None, SXZ, SYZ, SZZ, SYY)):
            str_[i, z] = q[z + 2, :, :LANES] if f is None else s[f - SXX, z + 2, :, :LANES]
        row = q[z + 2, Y0 : Y0 + 1, :LANES]
        slides = fp[1, z + 2 : z + 3, :LANES] > 0.5
        str_[1, z, Y0 : Y0 + 1, :] = jnp.where(slides, row - lists[0, z + 2 : z + 3, :LANES], row)


def along_strike(value, by):
    n = lax.axis_size("strike")
    return lax.ppermute(value, "strike", [(i, (i + by) % n) for i in range(n)])


def swapped(value, first):
    n = lax.axis_size("depth")
    pairs = [(i, i + 1) for i in range(first, n - 1, 2)]
    return lax.ppermute(value, "depth", pairs + [(j, i) for i, j in pairs])


def per_device(velocity, stress, b, lam, mu, past, coefs, pre, mask):
    edge = (7, NY, LANES)
    (owed,) = call(owed_kernel, [(STEPS, 8, LANES)], [coefs, past], smem=(0,))
    fields = jnp.concatenate([velocity, stress, DT * b[None], DT * lam[None], DT * mu[None]])
    to_next, to_prev = call(edges_kernel, [edge, edge], [fields, pre, mask, owed])
    from_prev = along_strike(to_next, 1)
    from_next = along_strike(to_prev, -1)
    v3, s5, q1, m3 = (3, 12, NY, EXT), (5, 12, NY, EXT), (12, NY, EXT), (3, 8, NY, EXT)
    edge, plane = (3, 2, NY, EXT), (ROWS, EXT)
    v, s, q, m, fp, lists, one, two = call(
        start_kernel,
        [v3, s5, q1, m3, (2, *plane), (STEPS, *plane)] + [(FIRST_TILES, NY, LANES)] * 2,
        [fields, pre, mask, owed, from_prev, from_next],
    )
    edge_m = m
    for step in range(0, STEPS, 2):
        first = step == 0
        one = swapped(one, 0)
        two = swapped(two, 1)
        left = STEPS - step - 1
        more = call(
            functools.partial(meet_kernel, first),
            [(left, *plane)] + ([edge, (2, *plane), (STEPS, *plane)] if first else []),
            [coefs, one, two, v, s, m, edge_m, fp, lists],
            smem=(0,),
            scratch=[pltpu.VMEM(plane, jnp.float32)],
        )
        if first:
            edge_m, fp, lists = more[1:]
        got = along_strike(more[0], 1)
        v, s, q, rates = call(
            functools.partial(two_steps_kernel, first),
            [v3, s5, q1, plane],
            [m, edge_m, fp, lists, one, two, v, s, q],
            {6: 0, 7: 1, 8: 2},
        )
        if step + 2 < STEPS:
            lists = along_strike(got[1:] + coefs[: left - 1, None, None] * rates[None], 1)
            v, q, one, two = call(
                part_kernel,
                [v3, q1] + [(TILES, NY, LANES)] * 2,
                [m, fp, got, s, v, q],
                {4: 0, 5: 1},
            )
    return tuple(call(end_kernel, [velocity.shape, stress.shape], [fp, got, v, s, q]))


def solution(mesh):
    placed = (
        P(None, "depth", None, "strike"),
        P(None, "depth", None, "strike"),
        P("depth", None, "strike"),
        P("depth", None, "strike"),
        P("depth", None, "strike"),
        P(None, "depth", "strike"),
        P(),
        P("depth", "strike"),
        P("depth", "strike"),
    )
    return jax.shard_map(
        per_device,
        mesh=mesh,
        in_specs=placed,
        out_specs=(P(None, "depth", None, "strike"), P(None, "depth", None, "strike")),
        check_vma=False,
    )
```

```python
import functools

import jax
import jax.numpy as jnp
from jax import lax
from jax.experimental import pallas as pl
from jax.experimental.pallas import tpu as pltpu
from jax.sharding import PartitionSpec as P


HIST = 64
STEPS = 8
DT = 0.3
FRIC = 0.5

NY = 32
Y0 = NY // 2
LANES = 128
EXT = 2 * LANES
W = STEPS
ROWS = 16
VMEM = pl.BlockSpec(memory_space=pltpu.VMEM)
SMEM = pl.BlockSpec(memory_space=pltpu.SMEM)

VX, VY, VZ, SXX, SXZ, SYZ, SZZ, SYY, SXY, B, LAM, MU = range(12)

TRACES = 6
TILES = TRACES + 1
FIRST = TRACES + 3
FIRST_TILES = FIRST + 3


def call(body, outs, ins, aliases=None, smem=(), scratch=()):
    return pl.pallas_call(
        body,
        out_shape=[jax.ShapeDtypeStruct(s, jnp.float32) for s in outs],
        in_specs=[SMEM if i in smem else VMEM for i in range(len(ins))],
        out_specs=[VMEM] * len(outs),
        scratch_shapes=scratch,
        input_output_aliases=aliases or {},
        compiler_params=pltpu.CompilerParams(vmem_limit_bytes=32 * 1024 * 1024),
        cost_estimate=pl.CostEstimate(flops=4_000_000, bytes_accessed=4_000_000, transcendentals=0),
    )(*ins)


def lane_of(rows):
    return lax.broadcasted_iota(jnp.int32, (rows, LANES), 1)


def rolled(tile, by):
    by %= LANES
    return tile if by == 0 else pltpu.roll(tile, by, 1)


def ahead_x(f):
    return pltpu.roll(f, f.shape[1] - 1, 1)


def behind_x(f):
    return pltpu.roll(f, 1, 1)


def ahead_y(f):
    row = lax.broadcasted_iota(jnp.int32, f.shape, 0)
    return jnp.where(row == NY - 1, 0.0, pltpu.roll(f, NY - 1, 0))


def behind_y(f):
    row = lax.broadcasted_iota(jnp.int32, f.shape, 0)
    return jnp.where(row == 0, 0.0, pltpu.roll(f, 1, 0))


def plane_of(refs, f, z):
    v, s, q, m = refs
    if f < SXX:
        return v.at[f, z]
    if f < SXY:
        return s.at[f - SXX, z]
    if f == SXY:
        return q.at[z]
    return m.at[f - B, z - 2]


def velocity_change(stress, z, b, want):
    sxy, sxz, syz, szz = stress(SXY, z), stress(SXZ, z), stress(SYZ, z), stress(SZZ, z)
    out = {}
    if VX in want:
        sxx = stress(SXX, z)
        out[VX] = b * ((ahead_x(sxx) - sxx) + (sxy - behind_y(sxy)) + (sxz - stress(SXZ, z - 1)))
    if VY in want:
        syy = stress(SYY, z)
        out[VY] = b * ((sxy - behind_x(sxy)) + (ahead_y(syy) - syy) + (syz - stress(SYZ, z - 1)))
    if VZ in want:
        out[VZ] = b * ((sxz - behind_x(sxz)) + (syz - behind_y(syz)) + (stress(SZZ, z + 1) - szz))
    return out


def stress_change(velocity, z, lam, mu, want):
    vx, vy, vz = velocity(VX, z), velocity(VY, z), velocity(VZ, z)
    ex = vx - behind_x(vx)
    ey = vy - behind_y(vy)
    ez = vz - velocity(VZ, z - 1)
    spread = lam * (ex + ey + ez)
    twice = mu + mu
    out = {}
    if SXX in want:
        out[SXX] = spread + twice * ex
        out[SYY] = spread + twice * ey
        out[SXY] = mu * ((ahead_y(vx) - vx) + (ahead_x(vy) - vy))
    out[SZZ] = spread + twice * ez
    out[SXZ] = mu * ((velocity(VX, z + 1) - vx) + (ahead_x(vz) - vz))
    out[SYZ] = mu * ((velocity(VY, z + 1) - vy) + (ahead_y(vz) - vz))
    return out


ALL_V = (VX, VY, VZ)
ALL_S = (SXX, SXZ, SYZ, SZZ, SYY, SXY)


def rate_at(v, z):
    return v[VX, z, Y0 + 1 : Y0 + 2, :] - v[VX, z, Y0 : Y0 + 1, :]


def slide(q, fp, z, traction):
    slides = fp[1, pl.ds(z, 1), :] > 0.5
    q[z, Y0 : Y0 + 1, :] = jnp.where(slides, traction, q[z, Y0 : Y0 + 1, :])


def slid(plane, fp, z, traction):
    row = lax.broadcasted_iota(jnp.int32, plane.shape, 0)
    return jnp.where((row == Y0) & (fp[1, z : z + 1, :] > 0.5), traction, plane)


def packed(planes):
    lane = lane_of(NY)
    out = [plane[:, :LANES] for plane in planes]
    for first in range(0, len(planes), 8):
        edges = jnp.zeros((NY, LANES), jnp.float32)
        for i, plane in enumerate(planes[first : first + 8]):
            moved = rolled(plane[:, LANES:], W + 2 * W * i)
            edges = jnp.where((lane >= 2 * W * i) & (lane < 2 * W * (i + 1)), moved, edges)
        out.append(edges)
    return out


def even_depth():
    return lax.axis_index("depth") % 2 == 0


def post(up, down, one, two):
    even = even_depth()
    for i, (u, d) in enumerate(zip(up, down, strict=True)):
        one[i] = jnp.where(even, d, u)
        two[i] = jnp.where(even, u, d)


class Got:
    def __init__(self, one, two, count):
        self.one, self.two, self.count, self.even = one, two, count, even_depth()

    def tile(self, above, i, rows):
        first, second = (self.one, self.two) if above else (self.two, self.one)
        return jnp.where(self.even, first[i, rows, :], second[i, rows, :])

    def plane(self, above, i, rows=slice(None)):
        edges = self.tile(above, self.count + i // 8, rows)
        return jnp.concatenate([self.tile(above, i, rows), rolled(edges, -(W + 2 * W * (i % 8)))], axis=1)


def traces(refs, fp):
    v, s, q, m = refs
    nothing = jnp.zeros((NY, EXT), jnp.float32)

    def alone(f, z):
        return v[f, z] if 2 <= z < 10 else nothing

    def before(f, z):
        return q[z] if f == SXY else s[f - SXX, z]

    def carried(z, want_s, want_v):
        now = {f: before(f, z) + c for f, c in stress_change(alone, z, m[1, z - 2], m[2, z - 2], want_s).items()}
        if SXY in now:
            now[SXY] = slid(now[SXY], fp, z, fp[0, z : z + 1, :] + FRIC * rate_at(v, z))
        change = velocity_change(lambda f, at: now.get(f, nothing) if at == z else nothing, z, m[0, z - 2], want_v)
        return now, {f: v[f, z] + c for f, c in change.items()}

    now, then = carried(2, ALL_S, (VX, VY))
    up = [v[VX, 2], v[VY, 2], before(SZZ, 2), now[SZZ], then[VX], then[VY]]
    now, then = carried(9, (SZZ, SXZ, SYZ), (VZ,))
    down = [before(SXZ, 9), before(SYZ, 9), v[VZ, 9], now[SXZ], now[SYZ], then[VZ]]
    return up, down


def owed_kernel(coefs, past, owed):
    for j in range(STEPS):
        parts = [None] * 4
        for k in range(HIST - j):
            term = coefs[j + k] * past[k]
            parts[k % 4] = term if parts[k % 4] is None else parts[k % 4] + term
        owed[j] = (parts[0] + parts[1]) + (parts[2] + parts[3])
    owed[STEPS] = jnp.full((8, LANES), coefs[0])


def edges_kernel(fields, pre, mask, owed, to_next, to_prev):
    lane8 = lane_of(8)
    nxt = jnp.zeros((8, LANES), jnp.float32)
    prv = jnp.zeros((8, LANES), jnp.float32)
    for i, plane in enumerate([owed[j] for j in range(STEPS)] + [pre[...], mask[...].astype(jnp.float32)]):
        here = (lane8 >= W * i) & (lane8 < W * (i + 1))
        nxt = jnp.where(here, rolled(plane, W * i - (LANES - W)), nxt)
        prv = jnp.where(here, rolled(plane, W * i), prv)
    to_next[6] = jnp.zeros((NY, LANES), jnp.float32)
    to_prev[6] = jnp.zeros((NY, LANES), jnp.float32)
    to_next[6, 0:8, :] = nxt
    to_prev[6, 0:8, :] = prv
    lane = lane_of(NY)
    for t in range(6):
        nxt = jnp.zeros((NY, LANES), jnp.float32)
        prv = jnp.zeros((NY, LANES), jnp.float32)
        for i in range(16):
            plane = fields[2 * t + i // 8, i % 8]
            here = (lane >= W * i) & (lane < W * (i + 1))
            nxt = jnp.where(here, rolled(plane, W * i - (LANES - W)), nxt)
            prv = jnp.where(here, rolled(plane, W * i), prv)
        to_next[t] = nxt
        to_prev[t] = prv


def move_first(refs, z, q_now=None):
    _, s, q, m = refs

    def stress(f, at):
        return (q if q_now is None else q_now)[at] if f == SXY else s[f - SXX, at]

    return velocity_change(stress, z, m[0, z - 2], ALL_V)


def start_kernel(fields, pre, mask, owed, from_prev, from_next, v, s, q, m, fp, lists, one, two, ahead):
    lane = lane_of(NY)
    lane8 = lane_of(8)
    empty = jnp.zeros((NY, EXT), jnp.float32)
    s[SXZ - SXX, 1] = empty
    s[SYZ - SXX, 1] = empty
    s[SZZ - SXX, 10] = empty
    refs = (v, s, q, m)
    for k, f in enumerate((VX, VY, VZ, SXX, SXY, SXZ, SYZ, SZZ, SYY, B, LAM, MU)):
        for z in range(8):
            at = (k % 2) * 8 + z
            edge = jnp.where(
                lane < LANES // 2,
                rolled(from_next[k // 2], -W * at),
                rolled(from_prev[k // 2], LANES - W - W * at),
            )
            to = plane_of(refs, f, z + 2)
            to[:, :LANES] = fields[k, z]
            to[:, LANES:] = edge
    fp[...] = jnp.zeros_like(fp)
    lists[...] = jnp.zeros_like(lists)
    for i in range(STEPS + 2):
        plane = owed[i] if i < STEPS else (pre, mask)[i - STEPS][...].astype(jnp.float32)
        edge = jnp.where(
            lane8 < LANES // 2,
            rolled(from_next[6, 0:8, :], -W * i),
            rolled(from_prev[6, 0:8, :], LANES - W - W * i),
        )
        to, j = (lists, i) if i < STEPS else (fp, i - STEPS)
        to[j, 2:10, :LANES] = plane
        to[j, 2:10, LANES:] = edge

    def step(z, carry):
        for f, change in move_first(refs, z).items():
            v[f, z] += change
        return carry

    lax.fori_loop(2, 10, step, 0, unroll=4)
    scale = jnp.concatenate([owed[STEPS, 0:1, :]] * 2, axis=1)
    ahead[...] = lists[1]
    for z in range(3, 10):
        ahead[z : z + 1, :] = lists[1, z : z + 1, :] + scale * rate_at(v, z)
    up, down = traces(refs, fp)
    up = packed(up + [m[k, 0] for k in range(3)])
    down = packed(down + [m[k, 7] for k in range(3)])
    post(up, down, one, two)
    last = len(up)
    one[last] = jnp.zeros((NY, LANES), jnp.float32)
    two[last] = jnp.zeros((NY, LANES), jnp.float32)
    for i in range(STEPS + 2):
        to, j = (lists, i) if i < STEPS else (fp, i - STEPS)
        for out in (one, two):
            out[last, i : i + 1, :] = to[j, 2:3, :LANES]
            out[last, 16 + i : 17 + i, :] = to[j, 2:3, LANES:]


def late_traction(fp, late, z):
    return jnp.where(fp[1, z : z + 1, :] > 0.5, -late[0, z : z + 1, :], 0.0)


def late_velocity(b, lack):
    row = lax.broadcasted_iota(jnp.int32, b.shape, 0)
    lack = jnp.broadcast_to(lack, b.shape)
    vx = jnp.where(row == Y0, b * lack, jnp.where(row == Y0 + 1, -(b * lack), 0.0))
    return vx, jnp.where(row == Y0, b * (lack - behind_x(lack)), 0.0)


def meet_kernel(first, coefs, one, two, v, s, m, edge_m, fp, lists, late, sent, *more):
    *more, rates = more
    got = Got(one, two, FIRST if first else TRACES)
    if first:
        edge_out, fp_out, lists_out = more
        for k in range(3):
            edge_out[k, 0] = got.plane(False, TRACES + k)
            edge_out[k, 1] = got.plane(True, TRACES + k)
        fp_out[...] = fp[...]
        lists_out[...] = lists[...]
        for i in range(STEPS + 2):
            to, j = (lists_out, i) if i < STEPS else (fp_out, i - STEPS)
            to[j, 10:11, :LANES] = got.tile(True, FIRST_TILES - 1, slice(i, i + 1))
            to[j, 10:11, LANES:] = got.tile(True, FIRST_TILES - 1, slice(16 + i, 17 + i))
        edge_m, lists = edge_out, lists_out
    rows = slice(Y0, Y0 + 8)
    rates[...] = jnp.zeros_like(rates)
    for z in range(2, 11):
        if z < 10:
            vx = v[VX, z, rows, :]
        else:
            vx = got.plane(True, 0, rows) - edge_m[0, 1, rows, :] * s[SXZ - SXX, 9, rows, :]
        if z == 2:
            vx = vx - m[0, 0, rows, :] * got.plane(False, 0, rows)
        rate = vx[1:2, :] - vx[0:1, :]
        if not first and z in (2, 10):
            b = m[0, 0, rows, :] if z == 2 else edge_m[0, 1, rows, :]
            rate = rate - (b[1:2, :] + b[0:1, :]) * late_traction(fp, late, z)
        rates[z : z + 1, :] = rate
    for j in range(sent.shape[0]):
        sent[j] = lists[j + 1] + coefs[j] * rates[...]


def two_steps_kernel(first, m, edge_m, fp, lists, late, one, two, v_in, s_in, q_in, v, s, q, rates):
    got = Got(one, two, FIRST if first else TRACES)
    sxz, syz, szz = SXZ - SXX, SYZ - SXX, SZZ - SXX
    nothing = jnp.zeros((NY, EXT), jnp.float32)
    if not first:
        late_own = late_velocity(m[0, 0], late_traction(fp, late, 2))
        late_above = late_velocity(edge_m[0, 1], late_traction(fp, late, 10))
    for z in range(2, 10):
        for f in ALL_V:
            plane = v_in[f, z]
            if z == 2 and f == VX:
                plane = plane - m[0, 0] * got.plane(False, 0)
            if z == 2 and f == VY:
                plane = plane - m[0, 0] * got.plane(False, 1)
            if z == 9 and f == VZ:
                plane = plane + m[0, 7] * got.plane(True, 2)
            if z == 2 and f < VZ and not first:
                plane = plane + late_own[f]
            v[f, z] = plane
    above = {VX: -(edge_m[0, 1] * s_in[sxz, 9]), VY: -(edge_m[0, 1] * s_in[syz, 9])}
    below = {VZ: edge_m[0, 0] * s_in[szz, 2]}
    if not first:
        above = {f: plane + late_above[f] for f, plane in above.items()}
    v[VX, 10] = got.plane(True, 0) + above[VX]
    v[VY, 10] = got.plane(True, 1) + above[VY]
    v[VZ, 1] = got.plane(False, 2) + below[VZ]
    more_above = stress_change(
        lambda f, z: above.get(f, nothing) if z == 10 else v[f, z] if z == 9 else nothing,
        10,
        edge_m[1, 1],
        edge_m[2, 1],
        ALL_S,
    )
    slip = above[VX][Y0 + 1 : Y0 + 2, :] - above[VX][Y0 : Y0 + 1, :]
    more_above[SXY] = slid(more_above[SXY], fp, 10, FRIC * slip - lists[0, 10:11, :])
    more_below = stress_change(
        lambda f, z: below.get(f, nothing) if z == 1 else v[f, z] if z == 2 else nothing,
        1,
        edge_m[1, 0],
        edge_m[2, 0],
        (SZZ, SXZ, SYZ),
    )
    s[szz, 10] = got.plane(True, 3) + more_above[SZZ]
    s[sxz, 1] = got.plane(False, 3) + more_below[SXZ]
    s[syz, 1] = got.plane(False, 4) + more_below[SYZ]

    def velocity(f, z):
        return v[f, z]

    def stress(f, z):
        return q[z] if f == SXY else s[f - SXX, z]

    def own_stress_a(z, carry):
        for f, change in stress_change(velocity, z, m[1, z - 2], m[2, z - 2], ALL_S).items():
            if f == SXY:
                q[z] = q_in[z] + change
            else:
                s[f - SXX, z] = s_in[f - SXX, z] + change
        slide(q, fp, z, fp[0, pl.ds(z, 1), :] + FRIC * rate_at(v, z) - lists[0, pl.ds(z, 1), :])
        return carry

    def own_velocity_b(z, carry):
        for f, change in velocity_change(stress, z, m[0, z - 2], ALL_V).items():
            v[f, z] += change
        return carry

    def own_stress_b(z, carry):
        for f, change in stress_change(velocity, z, m[1, z - 2], m[2, z - 2], ALL_S).items():
            if f == SXY:
                q[z] += change
            else:
                s[f - SXX, z] += change
        slide(q, fp, z, fp[0, pl.ds(z, 1), :] + FRIC * rate_at(v, z))
        return carry

    lax.fori_loop(2, 10, own_stress_a, 0, unroll=4)
    change = velocity_change(
        lambda f, z: more_above[f] if z == 10 else s[f - SXX, 9], 10, edge_m[0, 1], (VX, VY)
    )
    v[VX, 10] = got.plane(True, 4) + above[VX] + change[VX]
    v[VY, 10] = got.plane(True, 5) + above[VY] + change[VY]
    change = velocity_change(
        lambda f, z: more_below.get(f, nothing) if z == 1 else s[f - SXX, 2], 1, edge_m[0, 0], (VZ,)
    )
    v[VZ, 1] = got.plane(False, 5) + below[VZ] + change[VZ]
    lax.fori_loop(2, 10, own_velocity_b, 0, unroll=4)
    rates[...] = jnp.zeros_like(rates)
    for z in range(2, 11):
        rates[z : z + 1, :] = rate_at(v, z)
    lax.fori_loop(2, 10, own_stress_b, 0, unroll=4)
    s[sxz, 1] = nothing
    s[syz, 1] = nothing
    s[szz, 10] = nothing


def part_kernel(coefs, m, fp, ahead, near, s, v_in, q_in, v, q, one, two, rates):
    refs = (v, s, q, m)
    memory = ahead[...] if near is None else ahead[...] + coefs[0] * near[...]
    row = lax.broadcasted_iota(jnp.int32, memory.shape, 0)
    rates[...] = jnp.where(row > 2, memory, 0.0)

    def step(z, carry):
        q[z] = q_in[z]
        slide(q, fp, z, q[z, Y0 : Y0 + 1, :] - rates[pl.ds(z, 1), :])
        for f, change in move_first(refs, z).items():
            v[f, z] = v_in[f, z] + change
        return carry

    lax.fori_loop(2, 10, step, 0, unroll=4)
    up, down = traces(refs, fp)
    post(packed(up), packed(down), one, two)
    for z in range(3, 10):
        rates[z : z + 1, :] = rate_at(v, z)


def first_part_kernel(coefs, m, fp, ahead, *rest):
    part_kernel(coefs, m, fp, ahead, None, *rest)


def end_kernel(fp, lists, v, s, q, vel, str_):
    for z in range(8):
        for f in ALL_V:
            vel[f, z] = v[f, z + 2, :, :LANES]
        for i, f in enumerate((SXX, None, SXZ, SYZ, SZZ, SYY)):
            str_[i, z] = q[z + 2, :, :LANES] if f is None else s[f - SXX, z + 2, :, :LANES]
        row = q[z + 2, Y0 : Y0 + 1, :LANES]
        slides = fp[1, z + 2 : z + 3, :LANES] > 0.5
        str_[1, z, Y0 : Y0 + 1, :] = jnp.where(slides, row - lists[0, z + 2 : z + 3, :LANES], row)


def along_strike(value, by):
    n = lax.axis_size("strike")
    return lax.ppermute(value, "strike", [(i, (i + by) % n) for i in range(n)])


def swapped(value, first):
    n = lax.axis_size("depth")
    pairs = [(i, i + 1) for i in range(first, n - 1, 2)]
    return lax.ppermute(value, "depth", pairs + [(j, i) for i, j in pairs])


def per_device(velocity, stress, b, lam, mu, past, coefs, pre, mask):
    edge = (7, NY, LANES)
    (owed,) = call(owed_kernel, [(STEPS + 1, 8, LANES)], [coefs, past], smem=(0,))
    fields = jnp.concatenate([velocity, stress, DT * b[None], DT * lam[None], DT * mu[None]])
    to_next, to_prev = call(edges_kernel, [edge, edge], [fields, pre, mask, owed])
    from_prev = along_strike(to_next, 1)
    from_next = along_strike(to_prev, -1)
    v3, s5, q1, m3 = (3, 12, NY, EXT), (5, 12, NY, EXT), (12, NY, EXT), (3, 8, NY, EXT)
    edge, plane = (3, 2, NY, EXT), (ROWS, EXT)
    v, s, q, m, fp, lists, one, two, ahead = call(
        start_kernel,
        [v3, s5, q1, m3, (2, *plane), (STEPS, *plane)] + [(FIRST_TILES, NY, LANES)] * 2 + [plane],
        [fields, pre, mask, owed, from_prev, from_next],
    )
    edge_m = m
    late = lists
    ahead = along_strike(ahead, 1)
    for step in range(0, STEPS, 2):
        first = step == 0
        one = swapped(one, 0)
        two = swapped(two, 1)
        left = STEPS - step - 1
        more = call(
            functools.partial(meet_kernel, first),
            [(left, *plane)] + ([edge, (2, *plane), (STEPS, *plane)] if first else []),
            [coefs, one, two, v, s, m, edge_m, fp, lists, late],
            smem=(0,),
            scratch=[pltpu.VMEM(plane, jnp.float32)],
        )
        if first:
            edge_m, fp, lists = more[1:]
        got = along_strike(more[0], 1)
        v, s, q, rates = call(
            functools.partial(two_steps_kernel, first),
            [v3, s5, q1, plane],
            [m, edge_m, fp, lists, late, one, two, v, s, q],
            {7: 0, 8: 1, 9: 2},
        )
        if step + 2 < STEPS:
            v, q, one, two, ahead = call(
                first_part_kernel if first else part_kernel,
                [v3, q1] + [(TILES, NY, LANES)] * 2 + [plane],
                [coefs, m, fp, ahead] + ([] if first else [near]) + [s, v, q],
                {5: 0, 6: 1} if first else {6: 0, 7: 1},
                smem=(0,),
            )
        if step + 2 < STEPS:
            owed = got[1:] + coefs[: left - 1, None, None] * rates[None]
            lists = along_strike(jnp.concatenate([owed, ahead[None]]), 1)
            near = lists[left - 1]
            ahead = along_strike(owed[1], 2)
            late = got
    return tuple(call(end_kernel, [velocity.shape, stress.shape], [fp, got, v, s, q]))


def solution(mesh):
    placed = (
        P(None, "depth", None, "strike"),
        P(None, "depth", None, "strike"),
        P("depth", None, "strike"),
        P("depth", None, "strike"),
        P("depth", None, "strike"),
        P(None, "depth", "strike"),
        P(),
        P("depth", "strike"),
        P("depth", "strike"),
    )
    return jax.shard_map(
        per_device,
        mesh=mesh,
        in_specs=placed,
        out_specs=(P(None, "depth", None, "strike"), P(None, "depth", None, "strike")),
        check_vma=False,
    )
```

```python
import functools

import jax
import jax.numpy as jnp
from jax import lax
from jax.experimental import pallas as pl
from jax.experimental.pallas import tpu as pltpu
from jax.sharding import PartitionSpec as P


HIST = 64
STEPS = 8
DT = 0.3
FRIC = 0.5

NY = 32
Y0 = NY // 2
LANES = 128
EXT = 2 * LANES
W = STEPS
ROWS = 16
VMEM = pl.BlockSpec(memory_space=pltpu.VMEM)
SMEM = pl.BlockSpec(memory_space=pltpu.SMEM)

VX, VY, VZ, SXX, SXZ, SYZ, SZZ, SYY, SXY, B, LAM, MU = range(12)

TRACES = 6
TILES = TRACES + 1
FIRST = TRACES + 3
FIRST_TILES = FIRST + 3


def call(body, outs, ins, aliases=None, smem=(), scratch=()):
    return pl.pallas_call(
        body,
        out_shape=[jax.ShapeDtypeStruct(s, jnp.float32) for s in outs],
        in_specs=[SMEM if i in smem else VMEM for i in range(len(ins))],
        out_specs=[VMEM] * len(outs),
        scratch_shapes=scratch,
        input_output_aliases=aliases or {},
        compiler_params=pltpu.CompilerParams(vmem_limit_bytes=32 * 1024 * 1024),
        cost_estimate=pl.CostEstimate(flops=4_000_000, bytes_accessed=4_000_000, transcendentals=0),
    )(*ins)


def lane_of(rows):
    return lax.broadcasted_iota(jnp.int32, (rows, LANES), 1)


def rolled(tile, by):
    by %= LANES
    return tile if by == 0 else pltpu.roll(tile, by, 1)


def ahead_x(f):
    return pltpu.roll(f, f.shape[1] - 1, 1)


def behind_x(f):
    return pltpu.roll(f, 1, 1)


def ahead_y(f):
    row = lax.broadcasted_iota(jnp.int32, f.shape, 0)
    return jnp.where(row == NY - 1, 0.0, pltpu.roll(f, NY - 1, 0))


def behind_y(f):
    row = lax.broadcasted_iota(jnp.int32, f.shape, 0)
    return jnp.where(row == 0, 0.0, pltpu.roll(f, 1, 0))


def plane_of(refs, f, z):
    v, s, q, m = refs
    if f < SXX:
        return v.at[f, z]
    if f < SXY:
        return s.at[f - SXX, z]
    if f == SXY:
        return q.at[z]
    return m.at[f - B, z - 2]


def velocity_change(stress, z, b, want):
    sxy, sxz, syz, szz = stress(SXY, z), stress(SXZ, z), stress(SYZ, z), stress(SZZ, z)
    out = {}
    if VX in want:
        sxx = stress(SXX, z)
        out[VX] = b * ((ahead_x(sxx) - sxx) + (sxy - behind_y(sxy)) + (sxz - stress(SXZ, z - 1)))
    if VY in want:
        syy = stress(SYY, z)
        out[VY] = b * ((sxy - behind_x(sxy)) + (ahead_y(syy) - syy) + (syz - stress(SYZ, z - 1)))
    if VZ in want:
        out[VZ] = b * ((sxz - behind_x(sxz)) + (syz - behind_y(syz)) + (stress(SZZ, z + 1) - szz))
    return out


def stress_change(velocity, z, lam, mu, want):
    vx, vy, vz = velocity(VX, z), velocity(VY, z), velocity(VZ, z)
    ex = vx - behind_x(vx)
    ey = vy - behind_y(vy)
    ez = vz - velocity(VZ, z - 1)
    spread = lam * (ex + ey + ez)
    twice = mu + mu
    out = {}
    if SXX in want:
        out[SXX] = spread + twice * ex
        out[SYY] = spread + twice * ey
        out[SXY] = mu * ((ahead_y(vx) - vx) + (ahead_x(vy) - vy))
    out[SZZ] = spread + twice * ez
    out[SXZ] = mu * ((velocity(VX, z + 1) - vx) + (ahead_x(vz) - vz))
    out[SYZ] = mu * ((velocity(VY, z + 1) - vy) + (ahead_y(vz) - vz))
    return out


ALL_V = (VX, VY, VZ)
ALL_S = (SXX, SXZ, SYZ, SZZ, SYY, SXY)


def rate_at(v, z):
    return v[VX, z, Y0 + 1 : Y0 + 2, :] - v[VX, z, Y0 : Y0 + 1, :]


def slide(q, fp, z, traction):
    slides = fp[1, pl.ds(z, 1), :] > 0.5
    q[z, Y0 : Y0 + 1, :] = jnp.where(slides, traction, q[z, Y0 : Y0 + 1, :])


def slid(plane, fp, z, traction):
    row = lax.broadcasted_iota(jnp.int32, plane.shape, 0)
    return jnp.where((row == Y0) & (fp[1, z : z + 1, :] > 0.5), traction, plane)


def packed(planes):
    lane = lane_of(NY)
    out = [plane[:, :LANES] for plane in planes]
    for first in range(0, len(planes), 8):
        edges = jnp.zeros((NY, LANES), jnp.float32)
        for i, plane in enumerate(planes[first : first + 8]):
            moved = rolled(plane[:, LANES:], W + 2 * W * i)
            edges = jnp.where((lane >= 2 * W * i) & (lane < 2 * W * (i + 1)), moved, edges)
        out.append(edges)
    return out


def even_depth():
    return lax.axis_index("depth") % 2 == 0


def post(up, down, one, two):
    even = even_depth()
    for i, (u, d) in enumerate(zip(up, down, strict=True)):
        one[i] = jnp.where(even, d, u)
        two[i] = jnp.where(even, u, d)


class Got:
    def __init__(self, one, two, count):
        self.one, self.two, self.count, self.even = one, two, count, even_depth()

    def tile(self, above, i, rows):
        first, second = (self.one, self.two) if above else (self.two, self.one)
        return jnp.where(self.even, first[i, rows, :], second[i, rows, :])

    def plane(self, above, i, rows=slice(None)):
        edges = self.tile(above, self.count + i // 8, rows)
        return jnp.concatenate([self.tile(above, i, rows), rolled(edges, -(W + 2 * W * (i % 8)))], axis=1)


def traces(refs, fp):
    v, s, q, m = refs
    nothing = jnp.zeros((NY, EXT), jnp.float32)

    def alone(f, z):
        return v[f, z] if 2 <= z < 10 else nothing

    def before(f, z):
        return q[z] if f == SXY else s[f - SXX, z]

    def carried(z, want_s, want_v):
        now = {f: before(f, z) + c for f, c in stress_change(alone, z, m[1, z - 2], m[2, z - 2], want_s).items()}
        if SXY in now:
            now[SXY] = slid(now[SXY], fp, z, fp[0, z : z + 1, :] + FRIC * rate_at(v, z))
        change = velocity_change(lambda f, at: now.get(f, nothing) if at == z else nothing, z, m[0, z - 2], want_v)
        return now, {f: v[f, z] + c for f, c in change.items()}

    now, then = carried(2, ALL_S, (VX, VY))
    up = [v[VX, 2], v[VY, 2], before(SZZ, 2), now[SZZ], then[VX], then[VY]]
    now, then = carried(9, (SZZ, SXZ, SYZ), (VZ,))
    down = [before(SXZ, 9), before(SYZ, 9), v[VZ, 9], now[SXZ], now[SYZ], then[VZ]]
    return up, down


def owed_kernel(coefs, past, owed):
    sums = [[None, None] for _ in range(STEPS)]
    for k in range(HIST):
        plane = past[k]
        for j in range(min(STEPS, HIST - k)):
            old = sums[j][k % 2]
            term = coefs[j + k] * plane
            sums[j][k % 2] = term if old is None else old + term
    for j in range(STEPS):
        owed[j] = sums[j][0] + sums[j][1]
        owed[STEPS + j] = jnp.full((8, LANES), coefs[j])


def coef(owed, j):
    return jnp.concatenate([owed[STEPS + j, 0:1, :]] * 2, axis=1)


def edges_kernel(fields, pre, mask, owed, to_next, to_prev):
    lane8 = lane_of(8)
    nxt = jnp.zeros((8, LANES), jnp.float32)
    prv = jnp.zeros((8, LANES), jnp.float32)
    for i, plane in enumerate([owed[j] for j in range(STEPS)] + [pre[...], mask[...].astype(jnp.float32)]):
        here = (lane8 >= W * i) & (lane8 < W * (i + 1))
        nxt = jnp.where(here, rolled(plane, W * i - (LANES - W)), nxt)
        prv = jnp.where(here, rolled(plane, W * i), prv)
    to_next[6] = jnp.zeros((NY, LANES), jnp.float32)
    to_prev[6] = jnp.zeros((NY, LANES), jnp.float32)
    to_next[6, 0:8, :] = nxt
    to_prev[6, 0:8, :] = prv
    lane = lane_of(NY)
    for t in range(6):
        nxt = jnp.zeros((NY, LANES), jnp.float32)
        prv = jnp.zeros((NY, LANES), jnp.float32)
        for i in range(16):
            plane = fields[2 * t + i // 8, i % 8]
            here = (lane >= W * i) & (lane < W * (i + 1))
            nxt = jnp.where(here, rolled(plane, W * i - (LANES - W)), nxt)
            prv = jnp.where(here, rolled(plane, W * i), prv)
        to_next[t] = nxt
        to_prev[t] = prv


def move_first(refs, z, q_now=None):
    _, s, q, m = refs

    def stress(f, at):
        return (q if q_now is None else q_now)[at] if f == SXY else s[f - SXX, at]

    return velocity_change(stress, z, m[0, z - 2], ALL_V)


def start_kernel(fields, pre, mask, owed, from_prev, from_next, v, s, q, m, fp, lists, one, two, ahead):
    lane = lane_of(NY)
    lane8 = lane_of(8)
    empty = jnp.zeros((NY, EXT), jnp.float32)
    s[SXZ - SXX, 1] = empty
    s[SYZ - SXX, 1] = empty
    s[SZZ - SXX, 10] = empty
    refs = (v, s, q, m)
    for k, f in enumerate((SXX, SXY, SXZ, SYZ, SZZ, SYY, VX, VY, VZ, B, LAM, MU)):
        for z in range(8):
            at = (k % 2) * 8 + z
            edge = jnp.where(
                lane < LANES // 2,
                rolled(from_next[k // 2], -W * at),
                rolled(from_prev[k // 2], LANES - W - W * at),
            )
            to = plane_of(refs, f, z + 2)
            to[:, :LANES] = fields[k, z]
            to[:, LANES:] = edge
    fp[...] = jnp.zeros_like(fp)
    lists[...] = jnp.zeros_like(lists)
    for i in range(STEPS + 2):
        plane = owed[i] if i < STEPS else (pre, mask)[i - STEPS][...].astype(jnp.float32)
        edge = jnp.where(
            lane8 < LANES // 2,
            rolled(from_next[6, 0:8, :], -W * i),
            rolled(from_prev[6, 0:8, :], LANES - W - W * i),
        )
        to, j = (lists, i) if i < STEPS else (fp, i - STEPS)
        to[j, 2:10, :LANES] = plane
        to[j, 2:10, LANES:] = edge

    def step(z, carry):
        for f, change in move_first(refs, z).items():
            v[f, z] += change
        return carry

    lax.fori_loop(2, 10, step, 0, unroll=4)
    ahead[...] = lists[1]
    for z in range(3, 10):
        ahead[z : z + 1, :] = lists[1, z : z + 1, :] + coef(owed, 0) * rate_at(v, z)
    up, down = traces(refs, fp)
    up = packed(up + [m[k, 0] for k in range(3)])
    down = packed(down + [m[k, 7] for k in range(3)])
    post(up, down, one, two)
    last = len(up)
    one[last] = jnp.zeros((NY, LANES), jnp.float32)
    two[last] = jnp.zeros((NY, LANES), jnp.float32)
    for i in range(STEPS + 2):
        to, j = (lists, i) if i < STEPS else (fp, i - STEPS)
        for out in (one, two):
            out[last, i : i + 1, :] = to[j, 2:3, :LANES]
            out[last, 16 + i : 17 + i, :] = to[j, 2:3, LANES:]


def late_traction(fp, late, z):
    return jnp.where(fp[1, z : z + 1, :] > 0.5, -late[0, z : z + 1, :], 0.0)


def late_velocity(b, lack):
    row = lax.broadcasted_iota(jnp.int32, b.shape, 0)
    lack = jnp.broadcast_to(lack, b.shape)
    vx = jnp.where(row == Y0, b * lack, jnp.where(row == Y0 + 1, -(b * lack), 0.0))
    return vx, jnp.where(row == Y0, b * (lack - behind_x(lack)), 0.0)


def meet_kernel(first, owed, one, two, v, s, m, edge_m, fp, lists, late, sent, *more):
    *more, rates = more
    got = Got(one, two, FIRST if first else TRACES)
    if first:
        edge_out, fp_out, lists_out = more
        for k in range(3):
            edge_out[k, 0] = got.plane(False, TRACES + k)
            edge_out[k, 1] = got.plane(True, TRACES + k)
        fp_out[...] = fp[...]
        lists_out[...] = lists[...]
        for i in range(STEPS + 2):
            to, j = (lists_out, i) if i < STEPS else (fp_out, i - STEPS)
            to[j, 10:11, :LANES] = got.tile(True, FIRST_TILES - 1, slice(i, i + 1))
            to[j, 10:11, LANES:] = got.tile(True, FIRST_TILES - 1, slice(16 + i, 17 + i))
        edge_m, lists = edge_out, lists_out
    rows = slice(Y0, Y0 + 8)
    rates[...] = jnp.zeros_like(rates)
    for z in range(2, 11):
        if z < 10:
            vx = v[VX, z, rows, :]
        else:
            vx = got.plane(True, 0, rows) - edge_m[0, 1, rows, :] * s[SXZ - SXX, 9, rows, :]
        if z == 2:
            vx = vx - m[0, 0, rows, :] * got.plane(False, 0, rows)
        rate = vx[1:2, :] - vx[0:1, :]
        if not first and z in (2, 10):
            b = m[0, 0, rows, :] if z == 2 else edge_m[0, 1, rows, :]
            rate = rate - (b[1:2, :] + b[0:1, :]) * late_traction(fp, late, z)
        rates[z : z + 1, :] = rate
    for j in range(sent.shape[0]):
        sent[j] = lists[j + 1] + coef(owed, j) * rates[...]


def two_steps_kernel(first, m, edge_m, fp, lists, late, one, two, v_in, s_in, q_in, v, s, q, rates):
    got = Got(one, two, FIRST if first else TRACES)
    sxz, syz, szz = SXZ - SXX, SYZ - SXX, SZZ - SXX
    nothing = jnp.zeros((NY, EXT), jnp.float32)
    if not first:
        late_own = late_velocity(m[0, 0], late_traction(fp, late, 2))
        late_above = late_velocity(edge_m[0, 1], late_traction(fp, late, 10))
    for z in range(2, 10):
        for f in ALL_V:
            plane = v_in[f, z]
            if z == 2 and f == VX:
                plane = plane - m[0, 0] * got.plane(False, 0)
            if z == 2 and f == VY:
                plane = plane - m[0, 0] * got.plane(False, 1)
            if z == 9 and f == VZ:
                plane = plane + m[0, 7] * got.plane(True, 2)
            if z == 2 and f < VZ and not first:
                plane = plane + late_own[f]
            v[f, z] = plane
    above = {VX: -(edge_m[0, 1] * s_in[sxz, 9]), VY: -(edge_m[0, 1] * s_in[syz, 9])}
    below = {VZ: edge_m[0, 0] * s_in[szz, 2]}
    if not first:
        above = {f: plane + late_above[f] for f, plane in above.items()}
    v[VX, 10] = got.plane(True, 0) + above[VX]
    v[VY, 10] = got.plane(True, 1) + above[VY]
    v[VZ, 1] = got.plane(False, 2) + below[VZ]
    more_above = stress_change(
        lambda f, z: above.get(f, nothing) if z == 10 else v[f, z] if z == 9 else nothing,
        10,
        edge_m[1, 1],
        edge_m[2, 1],
        ALL_S,
    )
    slip = above[VX][Y0 + 1 : Y0 + 2, :] - above[VX][Y0 : Y0 + 1, :]
    more_above[SXY] = slid(more_above[SXY], fp, 10, FRIC * slip - lists[0, 10:11, :])
    more_below = stress_change(
        lambda f, z: below.get(f, nothing) if z == 1 else v[f, z] if z == 2 else nothing,
        1,
        edge_m[1, 0],
        edge_m[2, 0],
        (SZZ, SXZ, SYZ),
    )
    s[szz, 10] = got.plane(True, 3) + more_above[SZZ]
    s[sxz, 1] = got.plane(False, 3) + more_below[SXZ]
    s[syz, 1] = got.plane(False, 4) + more_below[SYZ]

    def velocity(f, z):
        return v[f, z]

    def stress(f, z):
        return q[z] if f == SXY else s[f - SXX, z]

    def own_stress_a(z, carry):
        for f, change in stress_change(velocity, z, m[1, z - 2], m[2, z - 2], ALL_S).items():
            if f == SXY:
                q[z] = q_in[z] + change
            else:
                s[f - SXX, z] = s_in[f - SXX, z] + change
        slide(q, fp, z, fp[0, pl.ds(z, 1), :] + FRIC * rate_at(v, z) - lists[0, pl.ds(z, 1), :])
        return carry

    def own_velocity_b(z, carry):
        for f, change in velocity_change(stress, z, m[0, z - 2], ALL_V).items():
            v[f, z] += change
        return carry

    def own_stress_b(z, carry):
        for f, change in stress_change(velocity, z, m[1, z - 2], m[2, z - 2], ALL_S).items():
            if f == SXY:
                q[z] += change
            else:
                s[f - SXX, z] += change
        slide(q, fp, z, fp[0, pl.ds(z, 1), :] + FRIC * rate_at(v, z))
        return carry

    lax.fori_loop(2, 10, own_stress_a, 0, unroll=4)
    change = velocity_change(
        lambda f, z: more_above[f] if z == 10 else s[f - SXX, 9], 10, edge_m[0, 1], (VX, VY)
    )
    v[VX, 10] = got.plane(True, 4) + above[VX] + change[VX]
    v[VY, 10] = got.plane(True, 5) + above[VY] + change[VY]
    change = velocity_change(
        lambda f, z: more_below.get(f, nothing) if z == 1 else s[f - SXX, 2], 1, edge_m[0, 0], (VZ,)
    )
    v[VZ, 1] = got.plane(False, 5) + below[VZ] + change[VZ]
    lax.fori_loop(2, 10, own_velocity_b, 0, unroll=4)
    rates[...] = jnp.zeros_like(rates)
    for z in range(2, 11):
        rates[z : z + 1, :] = rate_at(v, z)
    lax.fori_loop(2, 10, own_stress_b, 0, unroll=4)
    s[sxz, 1] = nothing
    s[syz, 1] = nothing
    s[szz, 10] = nothing


def part_kernel(owed, m, fp, ahead, near, s, v_in, q_in, v, q, one, two, rates):
    refs = (v, s, q, m)
    memory = ahead[...] if near is None else ahead[...] + coef(owed, 0) * near[...]
    row = lax.broadcasted_iota(jnp.int32, memory.shape, 0)
    rates[...] = jnp.where(row > 2, memory, 0.0)

    def step(z, carry):
        q[z] = q_in[z]
        slide(q, fp, z, q[z, Y0 : Y0 + 1, :] - rates[pl.ds(z, 1), :])
        for f, change in move_first(refs, z).items():
            v[f, z] = v_in[f, z] + change
        return carry

    lax.fori_loop(2, 10, step, 0, unroll=4)
    up, down = traces(refs, fp)
    post(packed(up), packed(down), one, two)
    for z in range(3, 10):
        rates[z : z + 1, :] = rate_at(v, z)


def first_part_kernel(owed, m, fp, ahead, *rest):
    part_kernel(owed, m, fp, ahead, None, *rest)


def end_kernel(fp, lists, v, s, q, vel, str_):
    for z in range(8):
        for f in ALL_V:
            vel[f, z] = v[f, z + 2, :, :LANES]
        for i, f in enumerate((SXX, None, SXZ, SYZ, SZZ, SYY)):
            str_[i, z] = q[z + 2, :, :LANES] if f is None else s[f - SXX, z + 2, :, :LANES]
        row = q[z + 2, Y0 : Y0 + 1, :LANES]
        slides = fp[1, z + 2 : z + 3, :LANES] > 0.5
        str_[1, z, Y0 : Y0 + 1, :] = jnp.where(slides, row - lists[0, z + 2 : z + 3, :LANES], row)


def along_strike(value, by):
    n = lax.axis_size("strike")
    return lax.ppermute(value, "strike", [(i, (i + by) % n) for i in range(n)])


def swapped(value, first):
    n = lax.axis_size("depth")
    pairs = [(i, i + 1) for i in range(first, n - 1, 2)]
    return lax.ppermute(value, "depth", pairs + [(j, i) for i, j in pairs])


def per_device(velocity, stress, b, lam, mu, past, coefs, pre, mask):
    edge = (7, NY, LANES)
    (owed,) = call(owed_kernel, [(2 * STEPS, 8, LANES)], [coefs, past], smem=(0,))
    fields = jnp.concatenate([stress, velocity, DT * b[None], DT * lam[None], DT * mu[None]])
    to_next, to_prev = call(edges_kernel, [edge, edge], [fields, pre, mask, owed])
    from_prev = along_strike(to_next, 1)
    from_next = along_strike(to_prev, -1)
    v3, s5, q1, m3 = (3, 12, NY, EXT), (5, 12, NY, EXT), (12, NY, EXT), (3, 8, NY, EXT)
    edge, plane = (3, 2, NY, EXT), (ROWS, EXT)
    v, s, q, m, fp, lists, one, two, ahead = call(
        start_kernel,
        [v3, s5, q1, m3, (2, *plane), (STEPS, *plane)] + [(FIRST_TILES, NY, LANES)] * 2 + [plane],
        [fields, pre, mask, owed, from_prev, from_next],
    )
    edge_m = m
    late = lists
    ahead = along_strike(ahead, 1)
    for step in range(0, STEPS, 2):
        first = step == 0
        one = swapped(one, 0)
        two = swapped(two, 1)
        left = STEPS - step - 1
        more = call(
            functools.partial(meet_kernel, first),
            [(left, *plane)] + ([edge, (2, *plane), (STEPS, *plane)] if first else []),
            [owed, one, two, v, s, m, edge_m, fp, lists, late],
            scratch=[pltpu.VMEM(plane, jnp.float32)],
        )
        if first:
            edge_m, fp, lists = more[1:]
        got = along_strike(more[0], 1)
        v, s, q, rates = call(
            functools.partial(two_steps_kernel, first),
            [v3, s5, q1, plane],
            [m, edge_m, fp, lists, late, one, two, v, s, q],
            {7: 0, 8: 1, 9: 2},
        )
        if step + 2 < STEPS:
            v, q, one, two, ahead = call(
                first_part_kernel if first else part_kernel,
                [v3, q1] + [(TILES, NY, LANES)] * 2 + [plane],
                [owed, m, fp, ahead] + ([] if first else [near]) + [s, v, q],
                {5: 0, 6: 1} if first else {6: 0, 7: 1},
            )
        if step + 2 < STEPS:
            next_lists = got[1:] + coefs[: left - 1, None, None] * rates[None]
            lists = along_strike(jnp.concatenate([next_lists, ahead[None]]), 1)
            near = lists[left - 1]
            ahead = along_strike(next_lists[1], 2)
            late = got
    return tuple(call(end_kernel, [velocity.shape, stress.shape], [fp, got, v, s, q]))


def solution(mesh):
    placed = (
        P(None, "depth", None, "strike"),
        P(None, "depth", None, "strike"),
        P("depth", None, "strike"),
        P("depth", None, "strike"),
        P("depth", None, "strike"),
        P(None, "depth", "strike"),
        P(),
        P("depth", "strike"),
        P("depth", "strike"),
    )
    return jax.shard_map(
        per_device,
        mesh=mesh,
        in_specs=placed,
        out_specs=(P(None, "depth", None, "strike"), P(None, "depth", None, "strike")),
        check_vma=False,
    )
```

```python
import functools

import jax
import jax.numpy as jnp
from jax import lax
from jax.experimental import pallas as pl
from jax.experimental.pallas import tpu as pltpu
from jax.sharding import PartitionSpec as P


HIST = 64
STEPS = 8
DT = 0.3
FRIC = 0.5

NY = 32
Y0 = NY // 2
LANES = 128
EXT = 2 * LANES
W = STEPS
ROWS = 16
VMEM = pl.BlockSpec(memory_space=pltpu.VMEM)
SMEM = pl.BlockSpec(memory_space=pltpu.SMEM)

VX, VY, VZ, SXX, SXZ, SYZ, SZZ, SYY, SXY, B, LAM, MU = range(12)

TRACES = 6
TILES = TRACES + 1
FIRST = TRACES + 3
FIRST_TILES = FIRST + 3


def call(body, outs, ins, aliases=None, smem=(), scratch=()):
    return pl.pallas_call(
        body,
        out_shape=[jax.ShapeDtypeStruct(s, jnp.float32) for s in outs],
        in_specs=[SMEM if i in smem else VMEM for i in range(len(ins))],
        out_specs=[VMEM] * len(outs),
        scratch_shapes=scratch,
        input_output_aliases=aliases or {},
        compiler_params=pltpu.CompilerParams(vmem_limit_bytes=32 * 1024 * 1024),
        cost_estimate=pl.CostEstimate(flops=4_000_000, bytes_accessed=4_000_000, transcendentals=0),
    )(*ins)


def lane_of(rows):
    return lax.broadcasted_iota(jnp.int32, (rows, LANES), 1)


def rolled(tile, by):
    by %= LANES
    return tile if by == 0 else pltpu.roll(tile, by, 1)


def ahead_x(f):
    return pltpu.roll(f, f.shape[1] - 1, 1)


def behind_x(f):
    return pltpu.roll(f, 1, 1)


def ahead_y(f):
    row = lax.broadcasted_iota(jnp.int32, f.shape, 0)
    return jnp.where(row == NY - 1, 0.0, pltpu.roll(f, NY - 1, 0))


def behind_y(f):
    row = lax.broadcasted_iota(jnp.int32, f.shape, 0)
    return jnp.where(row == 0, 0.0, pltpu.roll(f, 1, 0))


def plane_of(refs, f, z):
    v, s, q, m = refs
    if f < SXX:
        return v.at[f, z]
    if f < SXY:
        return s.at[f - SXX, z]
    if f == SXY:
        return q.at[z]
    return m.at[f - B, z - 2]


def velocity_change(stress, z, b, want):
    sxy, sxz, syz, szz = stress(SXY, z), stress(SXZ, z), stress(SYZ, z), stress(SZZ, z)
    out = {}
    if VX in want:
        sxx = stress(SXX, z)
        out[VX] = b * ((ahead_x(sxx) - sxx) + (sxy - behind_y(sxy)) + (sxz - stress(SXZ, z - 1)))
    if VY in want:
        syy = stress(SYY, z)
        out[VY] = b * ((sxy - behind_x(sxy)) + (ahead_y(syy) - syy) + (syz - stress(SYZ, z - 1)))
    if VZ in want:
        out[VZ] = b * ((sxz - behind_x(sxz)) + (syz - behind_y(syz)) + (stress(SZZ, z + 1) - szz))
    return out


def stress_change(velocity, z, lam, mu, want):
    vx, vy, vz = velocity(VX, z), velocity(VY, z), velocity(VZ, z)
    ex = vx - behind_x(vx)
    ey = vy - behind_y(vy)
    ez = vz - velocity(VZ, z - 1)
    spread = lam * (ex + ey + ez)
    twice = mu + mu
    out = {}
    if SXX in want:
        out[SXX] = spread + twice * ex
        out[SYY] = spread + twice * ey
        out[SXY] = mu * ((ahead_y(vx) - vx) + (ahead_x(vy) - vy))
    out[SZZ] = spread + twice * ez
    out[SXZ] = mu * ((velocity(VX, z + 1) - vx) + (ahead_x(vz) - vz))
    out[SYZ] = mu * ((velocity(VY, z + 1) - vy) + (ahead_y(vz) - vz))
    return out


ALL_V = (VX, VY, VZ)
ALL_S = (SXX, SXZ, SYZ, SZZ, SYY, SXY)


def rate_at(v, z):
    return v[VX, z, Y0 + 1 : Y0 + 2, :] - v[VX, z, Y0 : Y0 + 1, :]


def slide(q, fp, z, traction):
    slides = fp[1, pl.ds(z, 1), :] > 0.5
    q[z, Y0 : Y0 + 1, :] = jnp.where(slides, traction, q[z, Y0 : Y0 + 1, :])


def slid(plane, fp, z, traction):
    row = lax.broadcasted_iota(jnp.int32, plane.shape, 0)
    return jnp.where((row == Y0) & (fp[1, z : z + 1, :] > 0.5), traction, plane)


def packed(planes):
    lane = lane_of(NY)
    out = [plane[:, :LANES] for plane in planes]
    for first in range(0, len(planes), 8):
        edges = jnp.zeros((NY, LANES), jnp.float32)
        for i, plane in enumerate(planes[first : first + 8]):
            moved = rolled(plane[:, LANES:], W + 2 * W * i)
            edges = jnp.where((lane >= 2 * W * i) & (lane < 2 * W * (i + 1)), moved, edges)
        out.append(edges)
    return out


def even_depth():
    return lax.axis_index("depth") % 2 == 0


def post(up, down, one, two):
    even = even_depth()
    for i, (u, d) in enumerate(zip(up, down, strict=True)):
        one[i] = jnp.where(even, d, u)
        two[i] = jnp.where(even, u, d)


class Got:
    def __init__(self, one, two, count):
        self.one, self.two, self.count, self.even = one, two, count, even_depth()

    def tile(self, above, i, rows):
        first, second = (self.one, self.two) if above else (self.two, self.one)
        return jnp.where(self.even, first[i, rows, :], second[i, rows, :])

    def plane(self, above, i, rows=slice(None)):
        edges = self.tile(above, self.count + i // 8, rows)
        return jnp.concatenate([self.tile(above, i, rows), rolled(edges, -(W + 2 * W * (i % 8)))], axis=1)


def traces(refs, fp):
    v, s, q, m = refs
    nothing = jnp.zeros((NY, EXT), jnp.float32)

    def alone(f, z):
        return v[f, z] if 2 <= z < 10 else nothing

    def before(f, z):
        return q[z] if f == SXY else s[f - SXX, z]

    def carried(z, want_s, want_v):
        now = {f: before(f, z) + c for f, c in stress_change(alone, z, m[1, z - 2], m[2, z - 2], want_s).items()}
        if SXY in now:
            now[SXY] = slid(now[SXY], fp, z, fp[0, z : z + 1, :] + FRIC * rate_at(v, z))
        change = velocity_change(lambda f, at: now.get(f, nothing) if at == z else nothing, z, m[0, z - 2], want_v)
        return now, {f: v[f, z] + c for f, c in change.items()}

    now, then = carried(2, ALL_S, (VX, VY))
    up = [v[VX, 2], v[VY, 2], before(SZZ, 2), now[SZZ], then[VX], then[VY]]
    now, then = carried(9, (SZZ, SXZ, SYZ), (VZ,))
    down = [before(SXZ, 9), before(SYZ, 9), v[VZ, 9], now[SXZ], now[SYZ], then[VZ]]
    return up, down


def owed_kernel(coefs, past, owed):
    sums = [[None, None] for _ in range(STEPS)]
    for k in range(HIST):
        plane = past[k]
        for j in range(min(STEPS, HIST - k)):
            old = sums[j][k % 2]
            term = coefs[j + k : j + k + 1, :] * plane
            sums[j][k % 2] = term if old is None else old + term
    for j in range(STEPS):
        owed[j] = sums[j][0] + sums[j][1]
        owed[STEPS + j] = jnp.broadcast_to(coefs[j : j + 1, :], (8, LANES))


def coef(owed, j):
    return jnp.concatenate([owed[STEPS + j, 0:1, :]] * 2, axis=1)


def edges_kernel(fields, pre, mask, owed, to_next, to_prev):
    lane8 = lane_of(8)
    nxt = jnp.zeros((8, LANES), jnp.float32)
    prv = jnp.zeros((8, LANES), jnp.float32)
    for i, plane in enumerate([owed[j] for j in range(STEPS)] + [pre[...], mask[...].astype(jnp.float32)]):
        here = (lane8 >= W * i) & (lane8 < W * (i + 1))
        nxt = jnp.where(here, rolled(plane, W * i - (LANES - W)), nxt)
        prv = jnp.where(here, rolled(plane, W * i), prv)
    to_next[6] = jnp.zeros((NY, LANES), jnp.float32)
    to_prev[6] = jnp.zeros((NY, LANES), jnp.float32)
    to_next[6, 0:8, :] = nxt
    to_prev[6, 0:8, :] = prv
    lane = lane_of(NY)
    for t in range(6):
        nxt = jnp.zeros((NY, LANES), jnp.float32)
        prv = jnp.zeros((NY, LANES), jnp.float32)
        for i in range(16):
            plane = fields[2 * t + i // 8, i % 8]
            here = (lane >= W * i) & (lane < W * (i + 1))
            nxt = jnp.where(here, rolled(plane, W * i - (LANES - W)), nxt)
            prv = jnp.where(here, rolled(plane, W * i), prv)
        to_next[t] = nxt
        to_prev[t] = prv


def move_first(refs, z, q_now=None):
    _, s, q, m = refs

    def stress(f, at):
        return (q if q_now is None else q_now)[at] if f == SXY else s[f - SXX, at]

    return velocity_change(stress, z, m[0, z - 2], ALL_V)


def start_kernel(fields, pre, mask, owed, from_prev, from_next, v, s, q, m, fp, lists, one, two, ahead):
    lane = lane_of(NY)
    lane8 = lane_of(8)
    empty = jnp.zeros((NY, EXT), jnp.float32)
    s[SXZ - SXX, 1] = empty
    s[SYZ - SXX, 1] = empty
    s[SZZ - SXX, 10] = empty
    refs = (v, s, q, m)
    for k, f in enumerate((SXX, SXY, SXZ, SYZ, SZZ, SYY, VX, VY, VZ, B, LAM, MU)):
        for z in range(8):
            at = (k % 2) * 8 + z
            edge = jnp.where(
                lane < LANES // 2,
                rolled(from_next[k // 2], -W * at),
                rolled(from_prev[k // 2], LANES - W - W * at),
            )
            to = plane_of(refs, f, z + 2)
            to[:, :LANES] = fields[k, z]
            to[:, LANES:] = edge
    fp[...] = jnp.zeros_like(fp)
    lists[...] = jnp.zeros_like(lists)
    for i in range(STEPS + 2):
        plane = owed[i] if i < STEPS else (pre, mask)[i - STEPS][...].astype(jnp.float32)
        edge = jnp.where(
            lane8 < LANES // 2,
            rolled(from_next[6, 0:8, :], -W * i),
            rolled(from_prev[6, 0:8, :], LANES - W - W * i),
        )
        to, j = (lists, i) if i < STEPS else (fp, i - STEPS)
        to[j, 2:10, :LANES] = plane
        to[j, 2:10, LANES:] = edge

    def step(z, carry):
        for f, change in move_first(refs, z).items():
            v[f, z] += change
        return carry

    lax.fori_loop(2, 10, step, 0, unroll=8)
    ahead[...] = lists[1]
    for z in range(3, 10):
        ahead[z : z + 1, :] = lists[1, z : z + 1, :] + coef(owed, 0) * rate_at(v, z)
    up, down = traces(refs, fp)
    up = packed(up + [m[k, 0] for k in range(3)])
    down = packed(down + [m[k, 7] for k in range(3)])
    post(up, down, one, two)
    last = len(up)
    one[last] = jnp.zeros((NY, LANES), jnp.float32)
    two[last] = jnp.zeros((NY, LANES), jnp.float32)
    for i in range(STEPS + 2):
        to, j = (lists, i) if i < STEPS else (fp, i - STEPS)
        for out in (one, two):
            out[last, i : i + 1, :] = to[j, 2:3, :LANES]
            out[last, 16 + i : 17 + i, :] = to[j, 2:3, LANES:]


def late_traction(fp, late, z):
    return jnp.where(fp[1, z : z + 1, :] > 0.5, -late[0, z : z + 1, :], 0.0)


def late_velocity(b, lack):
    row = lax.broadcasted_iota(jnp.int32, b.shape, 0)
    lack = jnp.broadcast_to(lack, b.shape)
    vx = jnp.where(row == Y0, b * lack, jnp.where(row == Y0 + 1, -(b * lack), 0.0))
    return vx, jnp.where(row == Y0, b * (lack - behind_x(lack)), 0.0)


def meet_kernel(first, owed, one, two, v, s, m, edge_m, fp, lists, late, sent, *more):
    *more, rates = more
    got = Got(one, two, FIRST if first else TRACES)
    if first:
        edge_out, fp_out, lists_out = more
        for k in range(3):
            edge_out[k, 0] = got.plane(False, TRACES + k)
            edge_out[k, 1] = got.plane(True, TRACES + k)
        fp_out[...] = fp[...]
        lists_out[...] = lists[...]
        for i in range(STEPS + 2):
            to, j = (lists_out, i) if i < STEPS else (fp_out, i - STEPS)
            to[j, 10:11, :LANES] = got.tile(True, FIRST_TILES - 1, slice(i, i + 1))
            to[j, 10:11, LANES:] = got.tile(True, FIRST_TILES - 1, slice(16 + i, 17 + i))
        edge_m, lists = edge_out, lists_out
    rows = slice(Y0, Y0 + 8)
    rates[...] = jnp.zeros_like(rates)
    for z in range(2, 11):
        if z < 10:
            vx = v[VX, z, rows, :]
        else:
            vx = got.plane(True, 0, rows) - edge_m[0, 1, rows, :] * s[SXZ - SXX, 9, rows, :]
        if z == 2:
            vx = vx - m[0, 0, rows, :] * got.plane(False, 0, rows)
        rate = vx[1:2, :] - vx[0:1, :]
        if not first and z in (2, 10):
            b = m[0, 0, rows, :] if z == 2 else edge_m[0, 1, rows, :]
            rate = rate - (b[1:2, :] + b[0:1, :]) * late_traction(fp, late, z)
        rates[z : z + 1, :] = rate
    for j in range(sent.shape[0]):
        sent[j] = lists[j + 1] + coef(owed, j) * rates[...]


def two_steps_kernel(first, m, edge_m, fp, lists, late, one, two, v_in, s_in, q_in, v, s, q, rates):
    got = Got(one, two, FIRST if first else TRACES)
    sxz, syz, szz = SXZ - SXX, SYZ - SXX, SZZ - SXX
    nothing = jnp.zeros((NY, EXT), jnp.float32)
    if not first:
        late_own = late_velocity(m[0, 0], late_traction(fp, late, 2))
        late_above = late_velocity(edge_m[0, 1], late_traction(fp, late, 10))
    for z in range(2, 10):
        for f in ALL_V:
            plane = v_in[f, z]
            if z == 2 and f == VX:
                plane = plane - m[0, 0] * got.plane(False, 0)
            if z == 2 and f == VY:
                plane = plane - m[0, 0] * got.plane(False, 1)
            if z == 9 and f == VZ:
                plane = plane + m[0, 7] * got.plane(True, 2)
            if z == 2 and f < VZ and not first:
                plane = plane + late_own[f]
            v[f, z] = plane
    above = {VX: -(edge_m[0, 1] * s_in[sxz, 9]), VY: -(edge_m[0, 1] * s_in[syz, 9])}
    below = {VZ: edge_m[0, 0] * s_in[szz, 2]}
    if not first:
        above = {f: plane + late_above[f] for f, plane in above.items()}
    v[VX, 10] = got.plane(True, 0) + above[VX]
    v[VY, 10] = got.plane(True, 1) + above[VY]
    v[VZ, 1] = got.plane(False, 2) + below[VZ]
    more_above = stress_change(
        lambda f, z: above.get(f, nothing) if z == 10 else v[f, z] if z == 9 else nothing,
        10,
        edge_m[1, 1],
        edge_m[2, 1],
        ALL_S,
    )
    slip = above[VX][Y0 + 1 : Y0 + 2, :] - above[VX][Y0 : Y0 + 1, :]
    more_above[SXY] = slid(more_above[SXY], fp, 10, FRIC * slip - lists[0, 10:11, :])
    more_below = stress_change(
        lambda f, z: below.get(f, nothing) if z == 1 else v[f, z] if z == 2 else nothing,
        1,
        edge_m[1, 0],
        edge_m[2, 0],
        (SZZ, SXZ, SYZ),
    )
    s[szz, 10] = got.plane(True, 3) + more_above[SZZ]
    s[sxz, 1] = got.plane(False, 3) + more_below[SXZ]
    s[syz, 1] = got.plane(False, 4) + more_below[SYZ]

    def velocity(f, z):
        return v[f, z]

    def stress(f, z):
        return q[z] if f == SXY else s[f - SXX, z]

    def own_stress_a(z, carry):
        for f, change in stress_change(velocity, z, m[1, z - 2], m[2, z - 2], ALL_S).items():
            if f == SXY:
                q[z] = q_in[z] + change
            else:
                s[f - SXX, z] = s_in[f - SXX, z] + change
        slide(q, fp, z, fp[0, pl.ds(z, 1), :] + FRIC * rate_at(v, z) - lists[0, pl.ds(z, 1), :])
        return carry

    def own_velocity_b(z, carry):
        for f, change in velocity_change(stress, z, m[0, z - 2], ALL_V).items():
            v[f, z] += change
        return carry

    def own_stress_b(z, carry):
        for f, change in stress_change(velocity, z, m[1, z - 2], m[2, z - 2], ALL_S).items():
            if f == SXY:
                q[z] += change
            else:
                s[f - SXX, z] += change
        slide(q, fp, z, fp[0, pl.ds(z, 1), :] + FRIC * rate_at(v, z))
        return carry

    lax.fori_loop(2, 10, own_stress_a, 0, unroll=8)
    change = velocity_change(
        lambda f, z: more_above[f] if z == 10 else s[f - SXX, 9], 10, edge_m[0, 1], (VX, VY)
    )
    v[VX, 10] = got.plane(True, 4) + above[VX] + change[VX]
    v[VY, 10] = got.plane(True, 5) + above[VY] + change[VY]
    change = velocity_change(
        lambda f, z: more_below.get(f, nothing) if z == 1 else s[f - SXX, 2], 1, edge_m[0, 0], (VZ,)
    )
    v[VZ, 1] = got.plane(False, 5) + below[VZ] + change[VZ]
    lax.fori_loop(2, 10, own_velocity_b, 0, unroll=8)
    rates[...] = jnp.zeros_like(rates)
    for z in range(2, 11):
        rates[z : z + 1, :] = rate_at(v, z)
    lax.fori_loop(2, 10, own_stress_b, 0, unroll=8)
    s[sxz, 1] = nothing
    s[syz, 1] = nothing
    s[szz, 10] = nothing


def part_kernel(owed, m, fp, ahead, near, s, v_in, q_in, v, q, one, two, rates):
    refs = (v, s, q, m)
    memory = ahead[...] if near is None else ahead[...] + coef(owed, 0) * near[...]
    row = lax.broadcasted_iota(jnp.int32, memory.shape, 0)
    rates[...] = jnp.where(row > 2, memory, 0.0)

    def step(z, carry):
        q[z] = q_in[z]
        slide(q, fp, z, q[z, Y0 : Y0 + 1, :] - rates[pl.ds(z, 1), :])
        for f, change in move_first(refs, z).items():
            v[f, z] = v_in[f, z] + change
        return carry

    lax.fori_loop(2, 10, step, 0, unroll=8)
    up, down = traces(refs, fp)
    post(packed(up), packed(down), one, two)
    for z in range(3, 10):
        rates[z : z + 1, :] = rate_at(v, z)


def first_part_kernel(owed, m, fp, ahead, *rest):
    part_kernel(owed, m, fp, ahead, None, *rest)


def end_kernel(fp, lists, v, s, q, vel, str_):
    for z in range(8):
        for f in ALL_V:
            vel[f, z] = v[f, z + 2, :, :LANES]
        for i, f in enumerate((SXX, None, SXZ, SYZ, SZZ, SYY)):
            str_[i, z] = q[z + 2, :, :LANES] if f is None else s[f - SXX, z + 2, :, :LANES]
        row = q[z + 2, Y0 : Y0 + 1, :LANES]
        slides = fp[1, z + 2 : z + 3, :LANES] > 0.5
        str_[1, z, Y0 : Y0 + 1, :] = jnp.where(slides, row - lists[0, z + 2 : z + 3, :LANES], row)


def along_strike(value, by):
    n = lax.axis_size("strike")
    return lax.ppermute(value, "strike", [(i, (i + by) % n) for i in range(n)])


def swapped(value, first):
    n = lax.axis_size("depth")
    pairs = [(i, i + 1) for i in range(first, n - 1, 2)]
    return lax.ppermute(value, "depth", pairs + [(j, i) for i, j in pairs])


def per_device(velocity, stress, b, lam, mu, past, coefs, pre, mask):
    edge = (7, NY, LANES)
    rows = jnp.broadcast_to(coefs[:, None], (HIST, LANES))
    (owed,) = call(owed_kernel, [(2 * STEPS, 8, LANES)], [rows, past])
    fields = jnp.concatenate([stress, velocity, DT * b[None], DT * lam[None], DT * mu[None]])
    to_next, to_prev = call(edges_kernel, [edge, edge], [fields, pre, mask, owed])
    from_prev = along_strike(to_next, 1)
    from_next = along_strike(to_prev, -1)
    v3, s5, q1, m3 = (3, 12, NY, EXT), (5, 12, NY, EXT), (12, NY, EXT), (3, 8, NY, EXT)
    edge, plane = (3, 2, NY, EXT), (ROWS, EXT)
    v, s, q, m, fp, lists, one, two, ahead = call(
        start_kernel,
        [v3, s5, q1, m3, (2, *plane), (STEPS, *plane)] + [(FIRST_TILES, NY, LANES)] * 2 + [plane],
        [fields, pre, mask, owed, from_prev, from_next],
    )
    edge_m = m
    late = lists
    ahead = along_strike(ahead, 1)
    for step in range(0, STEPS, 2):
        first = step == 0
        one = swapped(one, 0)
        two = swapped(two, 1)
        left = STEPS - step - 1
        more = call(
            functools.partial(meet_kernel, first),
            [(left, *plane)] + ([edge, (2, *plane), (STEPS, *plane)] if first else []),
            [owed, one, two, v, s, m, edge_m, fp, lists, late],
            scratch=[pltpu.VMEM(plane, jnp.float32)],
        )
        if first:
            edge_m, fp, lists = more[1:]
        got = along_strike(more[0], 1)
        v, s, q, rates = call(
            functools.partial(two_steps_kernel, first),
            [v3, s5, q1, plane],
            [m, edge_m, fp, lists, late, one, two, v, s, q],
            {7: 0, 8: 1, 9: 2},
        )
        if step + 2 < STEPS:
            v, q, one, two, ahead = call(
                first_part_kernel if first else part_kernel,
                [v3, q1] + [(TILES, NY, LANES)] * 2 + [plane],
                [owed, m, fp, ahead] + ([] if first else [near]) + [s, v, q],
                {5: 0, 6: 1} if first else {6: 0, 7: 1},
            )
        if step + 2 < STEPS:
            next_lists = got[1:] + coefs[: left - 1, None, None] * rates[None]
            lists = along_strike(jnp.concatenate([next_lists, ahead[None]]), 1)
            near = lists[left - 1]
            ahead = along_strike(next_lists[1], 2)
            late = got
    return tuple(call(end_kernel, [velocity.shape, stress.shape], [fp, got, v, s, q]))


def solution(mesh):
    placed = (
        P(None, "depth", None, "strike"),
        P(None, "depth", None, "strike"),
        P("depth", None, "strike"),
        P("depth", None, "strike"),
        P("depth", None, "strike"),
        P(None, "depth", "strike"),
        P(),
        P("depth", "strike"),
        P("depth", "strike"),
    )
    return jax.shard_map(
        per_device,
        mesh=mesh,
        in_specs=placed,
        out_specs=(P(None, "depth", None, "strike"), P(None, "depth", None, "strike")),
        check_vma=False,
    )
```

```python
import functools

import jax
import jax.numpy as jnp
from jax import lax
from jax.experimental import pallas as pl
from jax.experimental.pallas import tpu as pltpu
from jax.sharding import PartitionSpec as P


HIST = 64
STEPS = 8
DT = 0.3
FRIC = 0.5

NY = 32
Y0 = NY // 2
LANES = 128
EXT = 2 * LANES
W = STEPS
ROWS = 16
VMEM = pl.BlockSpec(memory_space=pltpu.VMEM)
SMEM = pl.BlockSpec(memory_space=pltpu.SMEM)

VX, VY, VZ, SXX, SXZ, SYZ, SZZ, SYY, SXY, B, LAM, MU = range(12)

TRACES = 6
TILES = TRACES + 1
FIRST = TRACES + 3
FIRST_TILES = FIRST + 3


def call(body, outs, ins, aliases=None, smem=(), scratch=()):
    return pl.pallas_call(
        body,
        out_shape=[jax.ShapeDtypeStruct(s, jnp.float32) for s in outs],
        in_specs=[SMEM if i in smem else VMEM for i in range(len(ins))],
        out_specs=[VMEM] * len(outs),
        scratch_shapes=scratch,
        input_output_aliases=aliases or {},
        compiler_params=pltpu.CompilerParams(vmem_limit_bytes=32 * 1024 * 1024),
        cost_estimate=pl.CostEstimate(flops=4_000_000, bytes_accessed=4_000_000, transcendentals=0),
    )(*ins)


def lane_of(rows):
    return lax.broadcasted_iota(jnp.int32, (rows, LANES), 1)


def rolled(tile, by):
    by %= LANES
    return tile if by == 0 else pltpu.roll(tile, by, 1)


def in_slot(lane, i):
    first = W * i % LANES
    return (lane >= first) & (lane < first + W)


def ahead_x(f):
    return pltpu.roll(f, f.shape[1] - 1, 1)


def behind_x(f):
    return pltpu.roll(f, 1, 1)


def ahead_y(f):
    return jnp.concatenate([f[1:], jnp.zeros((1, f.shape[1]), jnp.float32)], axis=0)


def behind_y(f):
    return jnp.concatenate([jnp.zeros((1, f.shape[1]), jnp.float32), f[:-1]], axis=0)


def plane_of(refs, f, z):
    v, s, q, m = refs
    if f < SXX:
        return v.at[f, z]
    if f < SXY:
        return s.at[f - SXX, z]
    if f == SXY:
        return q.at[z]
    return m.at[f - B, z - 2]


def velocity_change(stress, z, b, want):
    sxy, sxz, syz, szz = stress(SXY, z), stress(SXZ, z), stress(SYZ, z), stress(SZZ, z)
    out = {}
    if VX in want:
        sxx = stress(SXX, z)
        out[VX] = b * ((ahead_x(sxx) - sxx) + (sxy - behind_y(sxy)) + (sxz - stress(SXZ, z - 1)))
    if VY in want:
        syy = stress(SYY, z)
        out[VY] = b * ((sxy - behind_x(sxy)) + (ahead_y(syy) - syy) + (syz - stress(SYZ, z - 1)))
    if VZ in want:
        out[VZ] = b * ((sxz - behind_x(sxz)) + (syz - behind_y(syz)) + (stress(SZZ, z + 1) - szz))
    return out


def stress_change(velocity, z, lam, mu, want):
    vx, vy, vz = velocity(VX, z), velocity(VY, z), velocity(VZ, z)
    ex = vx - behind_x(vx)
    ey = vy - behind_y(vy)
    ez = vz - velocity(VZ, z - 1)
    spread = lam * (ex + ey + ez)
    twice = mu + mu
    out = {}
    if SXX in want:
        out[SXX] = spread + twice * ex
        out[SYY] = spread + twice * ey
        out[SXY] = mu * ((ahead_y(vx) - vx) + (ahead_x(vy) - vy))
    out[SZZ] = spread + twice * ez
    out[SXZ] = mu * ((velocity(VX, z + 1) - vx) + (ahead_x(vz) - vz))
    out[SYZ] = mu * ((velocity(VY, z + 1) - vy) + (ahead_y(vz) - vz))
    return out


ALL_V = (VX, VY, VZ)
ALL_S = (SXX, SXZ, SYZ, SZZ, SYY, SXY)


def rate_at(v, z):
    return v[VX, z, Y0 + 1 : Y0 + 2, :] - v[VX, z, Y0 : Y0 + 1, :]


def slide(q, fp, z, traction):
    slides = fp[1, pl.ds(z, 1), :] > 0.5
    q[z, Y0 : Y0 + 1, :] = jnp.where(slides, traction, q[z, Y0 : Y0 + 1, :])


def slid(plane, fp, z, traction):
    row = lax.broadcasted_iota(jnp.int32, plane.shape, 0)
    return jnp.where((row == Y0) & (fp[1, z : z + 1, :] > 0.5), traction, plane)


def packed(planes):
    lane = lane_of(NY)
    out = [plane[:, :LANES] for plane in planes]
    for first in range(0, len(planes), 8):
        edges = jnp.zeros((NY, LANES), jnp.float32)
        for i, plane in enumerate(planes[first : first + 8]):
            moved = rolled(plane[:, LANES:], W + 2 * W * i)
            edges = jnp.where((lane >= 2 * W * i) & (lane < 2 * W * (i + 1)), moved, edges)
        out.append(edges)
    return out


def even_depth():
    return lax.axis_index("depth") % 2 == 0


def post(up, down, one, two):
    even = even_depth()
    for i, (u, d) in enumerate(zip(up, down, strict=True)):
        one[i] = jnp.where(even, d, u)
        two[i] = jnp.where(even, u, d)


class Got:
    def __init__(self, one, two, count):
        self.one, self.two, self.count, self.even = one, two, count, even_depth()

    def tile(self, above, i, rows):
        first, second = (self.one, self.two) if above else (self.two, self.one)
        return jnp.where(self.even, first[i, rows, :], second[i, rows, :])

    def plane(self, above, i, rows=slice(None)):
        edges = self.tile(above, self.count + i // 8, rows)
        return jnp.concatenate([self.tile(above, i, rows), rolled(edges, -(W + 2 * W * (i % 8)))], axis=1)


def traces(refs, fp):
    v, s, q, m = refs
    nothing = jnp.zeros((NY, EXT), jnp.float32)

    def alone(f, z):
        return v[f, z] if 2 <= z < 10 else nothing

    def before(f, z):
        return q[z] if f == SXY else s[f - SXX, z]

    def carried(z, want_s, want_v):
        now = {f: before(f, z) + c for f, c in stress_change(alone, z, m[1, z - 2], m[2, z - 2], want_s).items()}
        if SXY in now:
            now[SXY] = slid(now[SXY], fp, z, fp[0, z : z + 1, :] + FRIC * rate_at(v, z))
        change = velocity_change(lambda f, at: now.get(f, nothing) if at == z else nothing, z, m[0, z - 2], want_v)
        return now, {f: v[f, z] + c for f, c in change.items()}

    now, then = carried(2, ALL_S, (VX, VY))
    up = [v[VX, 2], v[VY, 2], before(SZZ, 2), now[SZZ], then[VX], then[VY]]
    now, then = carried(9, (SZZ, SXZ, SYZ), (VZ,))
    down = [before(SXZ, 9), before(SYZ, 9), v[VZ, 9], now[SXZ], now[SYZ], then[VZ]]
    return up, down


def owed_kernel(coefs, past, owed):
    sums = [[None, None] for _ in range(STEPS)]
    for k in range(HIST):
        plane = past[k]
        for j in range(min(STEPS, HIST - k)):
            old = sums[j][k % 2]
            term = coefs[j + k : j + k + 1, :] * plane
            sums[j][k % 2] = term if old is None else old + term
    for j in range(STEPS):
        owed[j] = sums[j][0] + sums[j][1]
        owed[STEPS + j] = jnp.broadcast_to(coefs[j : j + 1, :], (8, LANES))


def coef(owed, j):
    return jnp.concatenate([owed[STEPS + j, 0:1, :]] * 2, axis=1)


def edges_kernel(fields, pre, mask, owed, to_next, to_prev):
    lane8 = lane_of(8)
    nxt = jnp.zeros((8, LANES), jnp.float32)
    prv = jnp.zeros((8, LANES), jnp.float32)
    for i, plane in enumerate([owed[j] for j in range(STEPS)] + [pre[...], mask[...].astype(jnp.float32)]):
        moved = rolled(plane, W * (i + 1))
        nxt = jnp.where(in_slot(lane8, i), moved, nxt)
        prv = jnp.where(in_slot(lane8, i + 1), moved, prv)
    to_next[6] = jnp.zeros((NY, LANES), jnp.float32)
    to_prev[6] = jnp.zeros((NY, LANES), jnp.float32)
    to_next[6, 0:8, :] = nxt
    to_prev[6, 0:8, :] = prv
    lane = lane_of(NY)
    for t in range(6):
        nxt = jnp.zeros((NY, LANES), jnp.float32)
        prv = jnp.zeros((NY, LANES), jnp.float32)
        for i in range(16):
            plane = fields[2 * t + i // 8, i % 8]
            moved = rolled(plane, W * (i + 1))
            nxt = jnp.where(in_slot(lane, i), moved, nxt)
            prv = jnp.where(in_slot(lane, i + 1), moved, prv)
        to_next[t] = nxt
        to_prev[t] = prv


def move_first(refs, z, q_now=None):
    _, s, q, m = refs

    def stress(f, at):
        return (q if q_now is None else q_now)[at] if f == SXY else s[f - SXX, at]

    return velocity_change(stress, z, m[0, z - 2], ALL_V)


def start_kernel(fields, pre, mask, owed, from_prev, from_next, v, s, q, m, fp, lists, one, two, ahead):
    lane = lane_of(NY)
    lane8 = lane_of(8)
    empty = jnp.zeros((NY, EXT), jnp.float32)
    s[SXZ - SXX, 1] = empty
    s[SYZ - SXX, 1] = empty
    s[SZZ - SXX, 10] = empty
    refs = (v, s, q, m)
    for k, f in enumerate((SXX, SXY, SXZ, SYZ, SZZ, SYY, VX, VY, VZ, B, LAM, MU)):
        for z in range(8):
            at = (k % 2) * 8 + z
            edge = rolled(jnp.where(in_slot(lane, at + 1), from_next[k // 2], from_prev[k // 2]), -W * (at + 1))
            to = plane_of(refs, f, z + 2)
            to[:, :LANES] = fields[k, z]
            to[:, LANES:] = edge
    fp[...] = jnp.zeros_like(fp)
    lists[...] = jnp.zeros_like(lists)
    for i in range(STEPS + 2):
        plane = owed[i] if i < STEPS else (pre, mask)[i - STEPS][...].astype(jnp.float32)
        edge = rolled(jnp.where(in_slot(lane8, i + 1), from_next[6, 0:8, :], from_prev[6, 0:8, :]), -W * (i + 1))
        to, j = (lists, i) if i < STEPS else (fp, i - STEPS)
        to[j, 2:10, :LANES] = plane
        to[j, 2:10, LANES:] = edge

    def step(z, carry):
        for f, change in move_first(refs, z).items():
            v[f, z] += change
        return carry

    lax.fori_loop(2, 10, step, 0, unroll=8)
    ahead[...] = lists[1]
    for z in range(3, 10):
        ahead[z : z + 1, :] = lists[1, z : z + 1, :] + coef(owed, 0) * rate_at(v, z)
    up, down = traces(refs, fp)
    up = packed(up + [m[k, 0] for k in range(3)])
    down = packed(down + [m[k, 7] for k in range(3)])
    post(up, down, one, two)
    last = len(up)
    one[last] = jnp.zeros((NY, LANES), jnp.float32)
    two[last] = jnp.zeros((NY, LANES), jnp.float32)
    for i in range(STEPS + 2):
        to, j = (lists, i) if i < STEPS else (fp, i - STEPS)
        for out in (one, two):
            out[last, i : i + 1, :] = to[j, 2:3, :LANES]
            out[last, 16 + i : 17 + i, :] = to[j, 2:3, LANES:]


def late_traction(fp, late, z):
    return jnp.where(fp[1, z : z + 1, :] > 0.5, -late[0, z : z + 1, :], 0.0)


def late_velocity(b, lack):
    row = lax.broadcasted_iota(jnp.int32, b.shape, 0)
    lack = jnp.broadcast_to(lack, b.shape)
    vx = jnp.where(row == Y0, b * lack, jnp.where(row == Y0 + 1, -(b * lack), 0.0))
    return vx, jnp.where(row == Y0, b * (lack - behind_x(lack)), 0.0)


def meet_kernel(first, owed, one, two, v, s, m, edge_m, fp, lists, late, sent, *more):
    *more, rates = more
    got = Got(one, two, FIRST if first else TRACES)
    if first:
        edge_out, fp_out, lists_out = more
        for k in range(3):
            edge_out[k, 0] = got.plane(False, TRACES + k)
            edge_out[k, 1] = got.plane(True, TRACES + k)
        fp_out[...] = fp[...]
        lists_out[...] = lists[...]
        for i in range(STEPS + 2):
            to, j = (lists_out, i) if i < STEPS else (fp_out, i - STEPS)
            to[j, 10:11, :LANES] = got.tile(True, FIRST_TILES - 1, slice(i, i + 1))
            to[j, 10:11, LANES:] = got.tile(True, FIRST_TILES - 1, slice(16 + i, 17 + i))
        edge_m, lists = edge_out, lists_out
    rows = slice(Y0, Y0 + 8)
    rates[...] = jnp.zeros_like(rates)
    for z in range(2, 11):
        if z < 10:
            vx = v[VX, z, rows, :]
        else:
            vx = got.plane(True, 0, rows) - edge_m[0, 1, rows, :] * s[SXZ - SXX, 9, rows, :]
        if z == 2:
            vx = vx - m[0, 0, rows, :] * got.plane(False, 0, rows)
        rate = vx[1:2, :] - vx[0:1, :]
        if not first and z in (2, 10):
            b = m[0, 0, rows, :] if z == 2 else edge_m[0, 1, rows, :]
            rate = rate - (b[1:2, :] + b[0:1, :]) * late_traction(fp, late, z)
        rates[z : z + 1, :] = rate
    for j in range(sent.shape[0]):
        sent[j] = lists[j + 1] + coef(owed, j) * rates[...]


def two_steps_kernel(first, m, edge_m, fp, lists, late, one, two, v_in, s_in, q_in, v, s, q, rates):
    got = Got(one, two, FIRST if first else TRACES)
    sxz, syz, szz = SXZ - SXX, SYZ - SXX, SZZ - SXX
    nothing = jnp.zeros((NY, EXT), jnp.float32)
    if not first:
        late_own = late_velocity(m[0, 0], late_traction(fp, late, 2))
        late_above = late_velocity(edge_m[0, 1], late_traction(fp, late, 10))
    for z in range(2, 10):
        for f in ALL_V:
            plane = v_in[f, z]
            if z == 2 and f == VX:
                plane = plane - m[0, 0] * got.plane(False, 0)
            if z == 2 and f == VY:
                plane = plane - m[0, 0] * got.plane(False, 1)
            if z == 9 and f == VZ:
                plane = plane + m[0, 7] * got.plane(True, 2)
            if z == 2 and f < VZ and not first:
                plane = plane + late_own[f]
            v[f, z] = plane
    above = {VX: -(edge_m[0, 1] * s_in[sxz, 9]), VY: -(edge_m[0, 1] * s_in[syz, 9])}
    below = {VZ: edge_m[0, 0] * s_in[szz, 2]}
    if not first:
        above = {f: plane + late_above[f] for f, plane in above.items()}
    v[VX, 10] = got.plane(True, 0) + above[VX]
    v[VY, 10] = got.plane(True, 1) + above[VY]
    v[VZ, 1] = got.plane(False, 2) + below[VZ]
    more_above = stress_change(
        lambda f, z: above.get(f, nothing) if z == 10 else v[f, z] if z == 9 else nothing,
        10,
        edge_m[1, 1],
        edge_m[2, 1],
        ALL_S,
    )
    slip = above[VX][Y0 + 1 : Y0 + 2, :] - above[VX][Y0 : Y0 + 1, :]
    more_above[SXY] = slid(more_above[SXY], fp, 10, FRIC * slip - lists[0, 10:11, :])
    more_below = stress_change(
        lambda f, z: below.get(f, nothing) if z == 1 else v[f, z] if z == 2 else nothing,
        1,
        edge_m[1, 0],
        edge_m[2, 0],
        (SZZ, SXZ, SYZ),
    )
    s[szz, 10] = got.plane(True, 3) + more_above[SZZ]
    s[sxz, 1] = got.plane(False, 3) + more_below[SXZ]
    s[syz, 1] = got.plane(False, 4) + more_below[SYZ]

    def velocity(f, z):
        return v[f, z]

    def stress(f, z):
        return q[z] if f == SXY else s[f - SXX, z]

    def own_stress_a(z, carry):
        for f, change in stress_change(velocity, z, m[1, z - 2], m[2, z - 2], ALL_S).items():
            if f == SXY:
                q[z] = q_in[z] + change
            else:
                s[f - SXX, z] = s_in[f - SXX, z] + change
        slide(q, fp, z, fp[0, pl.ds(z, 1), :] + FRIC * rate_at(v, z) - lists[0, pl.ds(z, 1), :])
        return carry

    def own_velocity_b(z, carry):
        for f, change in velocity_change(stress, z, m[0, z - 2], ALL_V).items():
            v[f, z] += change
        return carry

    def own_stress_b(z, carry):
        for f, change in stress_change(velocity, z, m[1, z - 2], m[2, z - 2], ALL_S).items():
            if f == SXY:
                q[z] += change
            else:
                s[f - SXX, z] += change
        slide(q, fp, z, fp[0, pl.ds(z, 1), :] + FRIC * rate_at(v, z))
        return carry

    lax.fori_loop(2, 10, own_stress_a, 0, unroll=8)
    change = velocity_change(
        lambda f, z: more_above[f] if z == 10 else s[f - SXX, 9], 10, edge_m[0, 1], (VX, VY)
    )
    v[VX, 10] = got.plane(True, 4) + above[VX] + change[VX]
    v[VY, 10] = got.plane(True, 5) + above[VY] + change[VY]
    change = velocity_change(
        lambda f, z: more_below.get(f, nothing) if z == 1 else s[f - SXX, 2], 1, edge_m[0, 0], (VZ,)
    )
    v[VZ, 1] = got.plane(False, 5) + below[VZ] + change[VZ]
    lax.fori_loop(2, 10, own_velocity_b, 0, unroll=8)
    rates[...] = jnp.zeros_like(rates)
    for z in range(2, 11):
        rates[z : z + 1, :] = rate_at(v, z)
    lax.fori_loop(2, 10, own_stress_b, 0, unroll=8)
    s[sxz, 1] = nothing
    s[syz, 1] = nothing
    s[szz, 10] = nothing


def part_kernel(owed, m, fp, ahead, near, s, v_in, q_in, v, q, one, two, rates):
    refs = (v, s, q, m)
    memory = ahead[...] if near is None else ahead[...] + coef(owed, 0) * near[...]
    row = lax.broadcasted_iota(jnp.int32, memory.shape, 0)
    rates[...] = jnp.where(row > 2, memory, 0.0)

    def step(z, carry):
        q[z] = q_in[z]
        slide(q, fp, z, q[z, Y0 : Y0 + 1, :] - rates[pl.ds(z, 1), :])
        for f, change in move_first(refs, z).items():
            v[f, z] = v_in[f, z] + change
        return carry

    lax.fori_loop(2, 10, step, 0, unroll=8)
    up, down = traces(refs, fp)
    post(packed(up), packed(down), one, two)
    for z in range(3, 10):
        rates[z : z + 1, :] = rate_at(v, z)


def first_part_kernel(owed, m, fp, ahead, *rest):
    part_kernel(owed, m, fp, ahead, None, *rest)


def end_kernel(fp, lists, v, s, q, vel, str_):
    for z in range(8):
        for f in ALL_V:
            vel[f, z] = v[f, z + 2, :, :LANES]
        for i, f in enumerate((SXX, None, SXZ, SYZ, SZZ, SYY)):
            str_[i, z] = q[z + 2, :, :LANES] if f is None else s[f - SXX, z + 2, :, :LANES]
        row = q[z + 2, Y0 : Y0 + 1, :LANES]
        slides = fp[1, z + 2 : z + 3, :LANES] > 0.5
        str_[1, z, Y0 : Y0 + 1, :] = jnp.where(slides, row - lists[0, z + 2 : z + 3, :LANES], row)


def along_strike(value, by):
    n = lax.axis_size("strike")
    return lax.ppermute(value, "strike", [(i, (i + by) % n) for i in range(n)])


def swapped(value, first):
    n = lax.axis_size("depth")
    pairs = [(i, i + 1) for i in range(first, n - 1, 2)]
    return lax.ppermute(value, "depth", pairs + [(j, i) for i, j in pairs])


def per_device(velocity, stress, b, lam, mu, past, coefs, pre, mask):
    edge = (7, NY, LANES)
    rows = jnp.broadcast_to(coefs[:, None], (HIST, LANES))
    (owed,) = call(owed_kernel, [(2 * STEPS, 8, LANES)], [rows, past])
    fields = jnp.concatenate([stress, velocity, DT * b[None], DT * lam[None], DT * mu[None]])
    to_next, to_prev = call(edges_kernel, [edge, edge], [fields, pre, mask, owed])
    from_prev = along_strike(to_next, 1)
    from_next = along_strike(to_prev, -1)
    v3, s5, q1, m3 = (3, 12, NY, EXT), (5, 12, NY, EXT), (12, NY, EXT), (3, 8, NY, EXT)
    edge, plane = (3, 2, NY, EXT), (ROWS, EXT)
    v, s, q, m, fp, lists, one, two, ahead = call(
        start_kernel,
        [v3, s5, q1, m3, (2, *plane), (STEPS, *plane)] + [(FIRST_TILES, NY, LANES)] * 2 + [plane],
        [fields, pre, mask, owed, from_prev, from_next],
    )
    edge_m = m
    late = lists
    ahead = along_strike(ahead, 1)
    for step in range(0, STEPS, 2):
        first = step == 0
        one = swapped(one, 0)
        two = swapped(two, 1)
        left = STEPS - step - 1
        more = call(
            functools.partial(meet_kernel, first),
            [(left, *plane)] + ([edge, (2, *plane), (STEPS, *plane)] if first else []),
            [owed, one, two, v, s, m, edge_m, fp, lists, late],
            scratch=[pltpu.VMEM(plane, jnp.float32)],
        )
        if first:
            edge_m, fp, lists = more[1:]
        got = along_strike(more[0], 1)
        v, s, q, rates = call(
            functools.partial(two_steps_kernel, first),
            [v3, s5, q1, plane],
            [m, edge_m, fp, lists, late, one, two, v, s, q],
            {7: 0, 8: 1, 9: 2},
        )
        if step + 2 < STEPS:
            more_pairs = step + 4 < STEPS
            v, q, one, two, *ahead_out = call(
                first_part_kernel if first else part_kernel,
                [v3, q1] + [(TILES, NY, LANES)] * 2 + [plane] * more_pairs,
                [owed, m, fp, ahead] + ([] if first else [near]) + [s, v, q],
                {5: 0, 6: 1} if first else {6: 0, 7: 1},
                scratch=[] if more_pairs else [pltpu.VMEM(plane, jnp.float32)],
            )
        if step + 2 < STEPS:
            next_lists = got[1:] + coefs[: left - 1, None, None] * rates[None]
            if step + 4 < STEPS:
                lists = along_strike(jnp.concatenate([next_lists, ahead_out[0][None]]), 1)
                near = lists[left - 1]
                ahead = along_strike(next_lists[1], 2)
            else:
                lists = along_strike(next_lists, 1)
            late = got
    return tuple(call(end_kernel, [velocity.shape, stress.shape], [fp, got, v, s, q]))


def solution(mesh):
    placed = (
        P(None, "depth", None, "strike"),
        P(None, "depth", None, "strike"),
        P("depth", None, "strike"),
        P("depth", None, "strike"),
        P("depth", None, "strike"),
        P(None, "depth", "strike"),
        P(),
        P("depth", "strike"),
        P("depth", "strike"),
    )
    return jax.shard_map(
        per_device,
        mesh=mesh,
        in_specs=placed,
        out_specs=(P(None, "depth", None, "strike"), P(None, "depth", None, "strike")),
        check_vma=False,
    )
```
